32 devices in a mesh: kv: 2 (over core), seq: 16 (over z, y, x), dp: 1.
Axes of the slice: x: 2, y: 2, z: 4, core: 2. Of those that a mesh axis runs over, the one named last changes fastest.
Arguments:
- token_input_state: bfloat16 [4, 8192], P('dp'), may hold values from -6 to 6
- query_matrix: bfloat16 [8192, 2048], P('seq', 'kv'), may hold values from -0.0625 to 0.0625
- key_value_weight: bfloat16 [8192, 512], P('seq', 'kv'), may hold values from -0.5 to 0.5
- output_weight: bfloat16 [2048, 8192], P('kv', 'seq'), may hold values from -0.125 to 0.125
- key_cache_rows: bfloat16 [4, 2, 32768, 128], P('dp', 'kv', 'seq'), may hold values from -6000 to 6000, as said below
- value_cache_rows: bfloat16 [4, 2, 32768, 128], P('dp', 'kv', 'seq'), may hold values from -24 to 24
- live_lengths: int32 [4, 16], P('dp'), may hold values from 2 to 2048, as said below
- owner_shard: int32 [4], P('dp'), may hold values from 0 to 15
Outputs:
- layer_out: bfloat16 [4, 8192], P('dp', 'seq')
The draws below stay inside these ranges and needn't reach their ends.
Inputs may be any that keep to these rules, and one draw needn't show every extreme that they name: `live_lengths`: every block holds 2 to 2048 live slots; the owner's block of a sequence holds fewer than 2048; in every sequence some other block holds exactly 2048. `key_cache_rows`: bounded as stated.
All inputs are finite; a program needn't handle non-finite values.
Results may differ from the reference program's by a relative error of at most 0.015.
The reference program's roundings to bfloat16 on the way (of `attended`) count: a program that leaves them out, or rounds other values in their place, can miss the bound.
Values may be sent and summed in bfloat16 or wider, within the bound.
A program may use at most 64 MiB of HBM per device.

```python
import math
import jax
import jax.numpy as jnp
from jax import lax

MODEL_WIDTH = 8192
HEAD_SIZE = 128
QUERY_GROUP = 8
BATCH_SEQUENCES = 4
LENGTH_PER_PART = 2048
KEY_VALUE_HEADS = 2
HQ = 16
CACHE_LENGTH = 32768
N_SEQ = 16


def lengths_and_owner(key):
    inner = jax.random.fold_in(key, 4242)
    first_key, second_key, third_key, fourth_key, fifth_key = jax.random.split(inner, 5)
    owner_shard = jax.random.randint(first_key, (BATCH_SEQUENCES,), 0, N_SEQ)
    owner_shard = jnp.where(jnp.arange(BATCH_SEQUENCES) == 0, N_SEQ - 1, owner_shard)
    first_draw = jax.random.randint(second_key, (BATCH_SEQUENCES, N_SEQ), 0, LENGTH_PER_PART)
    second_draw = jax.random.randint(third_key, (BATCH_SEQUENCES, N_SEQ), 0, LENGTH_PER_PART)
    third_draw = jax.random.randint(fourth_key, (BATCH_SEQUENCES, N_SEQ), 0, LENGTH_PER_PART)
    skewed = first_draw * second_draw // LENGTH_PER_PART * third_draw // LENGTH_PER_PART
    lengths = 2 + skewed
    lengths = jnp.minimum(lengths, LENGTH_PER_PART - 1)
    column = jnp.arange(N_SEQ)[None, :]
    extra = jax.random.randint(fifth_key, (BATCH_SEQUENCES,), 0, N_SEQ - 1)
    full_shard = (owner_shard + 1 + extra) % N_SEQ
    lengths = jnp.where(column == full_shard[:, None], LENGTH_PER_PART, lengths)
    return (lengths.astype(jnp.int32), owner_shard.astype(jnp.int32))


def draw_live_lengths(key, part):
    lengths, owner_shard = lengths_and_owner(key)
    return lengths


def draw_owner_shard(key, part):
    lengths, owner_shard = lengths_and_owner(key)
    return owner_shard


def draw_key_cache_rows(key, part):
    inner = jax.random.fold_in(key, 77)
    noise_key = jax.random.fold_in(inner, 0)
    complete_shape = (BATCH_SEQUENCES, KEY_VALUE_HEADS, N_SEQ, LENGTH_PER_PART, HEAD_SIZE)
    random_basis = jnp.clip(2.5 * jax.random.normal(noise_key, complete_shape, jnp.float32), -15.0, 15.0)
    return random_basis.reshape(BATCH_SEQUENCES, KEY_VALUE_HEADS, CACHE_LENGTH, HEAD_SIZE).astype(jnp.bfloat16)


def block_levels(rng, dims, shards, low, top_value):
    def one(dim, parts):
        steps = jax.random.uniform(jax.random.fold_in(jax.random.fold_in(rng, 6), dim), (parts,), jnp.float32, low / len(shards), top_value / len(shards))
        return jnp.repeat(jnp.exp(steps), dims[dim] // parts).reshape((-1,) + (1,) * (len(dims) - dim - 1))

    loudness = one(*shards[0])
    for cut in shards[1:]:
        loudness = loudness * one(*cut)
    return loudness


def normal_values(rng, shape, deviation, limit, cuts=(), held_as=jnp.bfloat16):
    factor_of = block_levels(rng, shape, cuts, -0.22, 0.18) if cuts else 1.0
    drawn = jax.random.normal(rng, shape, jnp.float32) * deviation * factor_of
    return jnp.minimum(jnp.maximum(drawn, -limit), limit).astype(held_as)


def setup_inputs(seed: int = 0, part: int = 0) -> dict:
    keys = jax.random.split(jax.random.key(seed), 9)
    part_splits = jax.random.split(jax.random.fold_in(keys[8], part), 9)
    token_input_state = normal_values(part_splits[0], (BATCH_SEQUENCES, MODEL_WIDTH), 1.0, 6.0)
    query_matrix = normal_values(keys[1], (MODEL_WIDTH, HQ * HEAD_SIZE), MODEL_WIDTH ** -0.5, 0.0625, ((0, 16), (1, 2)))
    key_value_weight = normal_values(keys[2], (MODEL_WIDTH, KEY_VALUE_HEADS * 2 * HEAD_SIZE), (MODEL_WIDTH // 64) ** -0.5, 0.5, ((0, 16), (1, 2)))
    output_weight = normal_values(keys[3], (HQ * HEAD_SIZE, MODEL_WIDTH), (HQ * HEAD_SIZE) ** -0.5, 0.125, ((0, 2), (1, 16)))
    key_cache_rows = draw_key_cache_rows(jax.random.fold_in(jax.random.fold_in(keys[8], part), 71), part)
    value_cache_rows = normal_values(part_splits[5], (BATCH_SEQUENCES, KEY_VALUE_HEADS, CACHE_LENGTH, HEAD_SIZE), 4.0, 24.0, ((1, 2), (2, 16)))
    live_lengths = draw_live_lengths(jax.random.fold_in(jax.random.fold_in(keys[8], part), 71), part)
    owner_shard = draw_owner_shard(jax.random.fold_in(jax.random.fold_in(keys[8], part), 71), part)
    return {"token_input_state": token_input_state, "query_matrix": query_matrix, "key_value_weight": key_value_weight, "output_weight": output_weight, "key_cache_rows": key_cache_rows, "value_cache_rows": value_cache_rows, "live_lengths": live_lengths, "owner_shard": owner_shard}


rope_theta = 500000.0

def frequencies():
    exponent = jnp.arange(0, HEAD_SIZE, 2).astype(jnp.float32) / HEAD_SIZE
    return jnp.power(rope_theta, -exponent)

def rotate(vectors, angles):
    half_size = vectors.shape[-1] // 2
    first_half = vectors[..., :half_size]
    second_half = vectors[..., half_size:]
    cosine_table = jnp.cos(angles)
    sine_table = jnp.sin(angles)
    return jnp.concatenate([first_half * cosine_table - second_half * sine_table, second_half * cosine_table + first_half * sine_table], -1)

def reference(token_input_state, query_matrix, key_value_weight, output_weight, key_cache_rows, value_cache_rows, live_lengths, owner_shard):
    query_rows = jnp.dot(token_input_state, query_matrix, preferred_element_type=jnp.float32).reshape(BATCH_SEQUENCES, KEY_VALUE_HEADS, QUERY_GROUP, HEAD_SIZE)
    key_value_rows = jnp.dot(token_input_state, key_value_weight, preferred_element_type=jnp.float32).reshape(BATCH_SEQUENCES, KEY_VALUE_HEADS, 2, HEAD_SIZE)
    lookup = jnp.take_along_axis(live_lengths, owner_shard[:, None].astype(jnp.int32), 1)[:, 0]
    position = owner_shard * LENGTH_PER_PART + lookup
    angles = position.astype(jnp.float32)[:, None] * frequencies()[None, :]
    query_rot = rotate(query_rows, angles[:, None, None, :]).astype(jnp.bfloat16)
    key_new = rotate(key_value_rows[:, :, 0], angles[:, None, :]).astype(jnp.bfloat16)
    value_new = key_value_rows[:, :, 1].astype(jnp.bfloat16)
    scaling = 1.0 / math.sqrt(HEAD_SIZE)
    key_rows = key_cache_rows.reshape(BATCH_SEQUENCES, KEY_VALUE_HEADS, N_SEQ, LENGTH_PER_PART, HEAD_SIZE)
    value_rows = value_cache_rows.reshape(BATCH_SEQUENCES, KEY_VALUE_HEADS, N_SEQ, LENGTH_PER_PART, HEAD_SIZE)
    scores = jnp.einsum('bhgd,bhsld->bhgsl', query_rot.astype(jnp.float32), key_rows.astype(jnp.float32)) * scaling
    slot_ids = jnp.arange(LENGTH_PER_PART)
    live_mask = slot_ids[None, None, :] < live_lengths[:, :, None]
    scores = jnp.where(live_mask[:, None, None], scores, -jnp.inf)
    new_score = lax.optimization_barrier(jnp.sum(query_rot.astype(jnp.float32) * key_new.astype(jnp.float32)[:, :, None, :], -1)) * scaling
    owner_mask = (owner_shard[:, None] == jnp.arange(N_SEQ)[None, :])[:, None, None, :]
    new_term = jnp.where(owner_mask, new_score[..., None], -jnp.inf)
    shard_top = jnp.maximum(lax.optimization_barrier(jnp.max(scores, -1)), new_term)
    probs = jnp.exp(scores - shard_top[..., None]).astype(jnp.bfloat16)
    new_prob = jnp.where(owner_mask, jnp.exp(new_score[..., None] - shard_top), 0.0).astype(jnp.bfloat16)
    totals = lax.optimization_barrier(jnp.sum(probs.astype(jnp.float32), -1)) + new_prob.astype(jnp.float32)
    accum = jnp.einsum('bhgsl,bhsld->bhgsd', probs.astype(jnp.float32), value_rows.astype(jnp.float32))
    accum = accum + new_prob.astype(jnp.float32)[..., None] * value_new.astype(jnp.float32)[:, :, None, None, :]
    overall = lax.optimization_barrier(jnp.max(shard_top, -1))
    factor = jnp.exp(shard_top - overall[..., None])
    attended = lax.optimization_barrier(jnp.sum(accum * factor[..., None], 3)) / lax.optimization_barrier(jnp.sum(totals * factor, 3))[..., None]
    attended = attended.astype(jnp.bfloat16).reshape(BATCH_SEQUENCES, HQ * HEAD_SIZE)
    return jnp.dot(attended, output_weight, preferred_element_type=jnp.float32).astype(jnp.bfloat16)
```

```python
import functools
import math

import jax
import jax.numpy as jnp
import numpy as np
from jax import lax
from jax.experimental import pallas as pl
from jax.experimental.pallas import tpu as pltpu
from jax.sharding import PartitionSpec as P

ROPE_THETA = 500000.0
F32 = jnp.float32
BF16 = jnp.bfloat16
MESH = pl.DeviceIdType.MESH
CHUNKS = 2


def kernel(
    n, inner, outer, group, head,
    live_hbm, owner_hbm, freq_hbm, x_hbm, wq_hbm, wkv_hbm, wo_hbm, k_hbm, v_hbm,
    out,
    live, owner, freq, x, wq, wkv, wo, keys, keys_t, vals,
    part, a_in, a_sum, b_in, acc_out, acc_in, stat_out, stat_in, kv_buf, att_rows,
    load_sem, a_recv, b_recv, g_recv, send_sem, stat_recv, wo_recv, kv_recv, ready,
):
    me = lax.axis_index("seq")
    kv = lax.axis_index("kv")
    other = 1 - kv
    batch = x.shape[0]
    rows = wq.shape[0]
    qw = wq.shape[1]
    slots = keys.shape[2]
    per = batch // CHUNKS
    pairs = batch * group
    plane = me // inner
    spot = lax.rem(me, inner)
    partner = {"kv": other}
    steps = [1 << i for i in range(outer.bit_length() - 1)]

    def flipped(j):
        return {"seq": j, "kv": other}

    def across(step):
        return {"seq": (plane + step - 2 * step * lax.rem(plane // step, 2)) * inner + spot}

    def signal(sem, device):
        pl.semaphore_signal(sem, inc=1, device_id=device, device_id_type=MESH)

    def push(src, dst, send, recv, device):
        pltpu.make_async_remote_copy(
            src_ref=src, dst_ref=dst, send_sem=send, recv_sem=recv,
            device_id=device, device_id_type=MESH,
        ).start()

    def arrived(buf, recv):
        pltpu.make_async_remote_copy(
            src_ref=buf, dst_ref=buf, send_sem=send_sem.at[0], recv_sem=recv,
            device_id=partner, device_id_type=MESH,
        ).wait_recv()

    def sent(buf, send):
        pltpu.make_async_remote_copy(
            src_ref=buf, dst_ref=buf, send_sem=send, recv_sem=a_recv.at[0],
            device_id=partner, device_id_type=MESH,
        ).wait_send()

    first = pl.multiple_of(me * rows, rows)
    half = rows // 2
    loads = [
        pltpu.make_async_copy(x_hbm.at[:, pl.ds(first, rows)], x, load_sem.at[0]),
        pltpu.make_async_copy(wq_hbm.at[pl.ds(0, half)], wq.at[pl.ds(0, half)], load_sem.at[1]),
        pltpu.make_async_copy(wq_hbm.at[pl.ds(half, half)], wq.at[pl.ds(half, half)], load_sem.at[2]),
        pltpu.make_async_copy(wkv_hbm, wkv, load_sem.at[3]),
        pltpu.make_async_copy(live_hbm, live, load_sem.at[4]),
        pltpu.make_async_copy(owner_hbm, owner, load_sem.at[5]),
        pltpu.make_async_copy(freq_hbm, freq, load_sem.at[6]),
        pltpu.make_async_copy(k_hbm, keys, load_sem.at[7]),
        pltpu.make_async_copy(v_hbm, vals, load_sem.at[8]),
    ]
    for cp in loads[:7]:
        cp.start()

    barrier = pltpu.get_barrier_semaphore()
    signal(barrier, partner)
    for d in range(1, inner):
        signal(barrier, flipped(plane * inner + lax.rem(spot + d, inner)))
    for step in steps:
        signal(barrier, across(step))

    loads[0].wait()
    loads[1].wait()
    low = jnp.dot(x[:, :half], wq[:half, :], preferred_element_type=F32)
    loads[2].wait()
    loads[3].wait()
    loads[7].start()
    loads[8].start()
    projected = low + jnp.dot(x[:, half:], wq[half:, :], preferred_element_type=F32)
    both = jnp.dot(x[...], wkv[...], preferred_element_type=F32)
    for h in range(group):
        part[:, h, :] = projected[:, h * head:(h + 1) * head]
    part[:, group, :] = both[:, :head]
    part[:, group + 1, :] = both[:, head:]
    pl.semaphore_wait(barrier, inner + len(steps))

    for c in range(CHUNKS):
        for d in list(range(1, inner)) + [0]:
            j = plane * inner + lax.rem(spot + d, inner)
            push(part.at[pl.ds(c * per, per)], a_in.at[c, spot], send_sem.at[0], a_recv.at[c], flipped(j))

    for cp in loads[4:7]:
        cp.wait()
    row_id = lax.broadcasted_iota(jnp.int32, (batch, head), 0)
    lane_id = lax.broadcasted_iota(jnp.int32, (batch, head), 1)
    position = jnp.zeros((batch, head), jnp.int32)
    for b in range(batch):
        own = owner[b]
        position = jnp.where(row_id == b, own * slots + live[b, own], position)
    angle = position.astype(F32) * freq[...]
    cosine = jnp.cos(angle)
    sine = jnp.sin(angle)
    sine = jnp.where(lane_id < head // 2, -sine, sine)

    def rotate(v, b):
        return v * cosine[b:b + 1] + pltpu.roll(v, head // 2, 1) * sine[b:b + 1]

    for i in range(max(len(steps) - 1, 1)):
        for step in steps:
            signal(ready.at[2 + i], across(step))
        if i == 0:
            loads[7].wait()
            for b in range(batch):
                keys_t[b] = keys[b, 0].T
        pl.semaphore_wait(ready.at[2 + i], len(steps))
    signal(ready.at[0], partner)
    pl.semaphore_wait(ready.at[0], 1)

    for c in range(CHUNKS):
        arrived(a_in.at[c], a_recv.at[c])
        total = a_in[c, 0]
        for j in range(1, inner):
            total = total + a_in[c, j]
        a_sum[c * per:(c + 1) * per] = total
        for d in list(range(1, outer)) + [0]:
            j = lax.rem(plane + d, outer) * inner + spot
            push(a_sum.at[pl.ds(c * per, per)], b_in.at[c, plane], send_sem.at[1], b_recv.at[c], flipped(j))
    push(wo_hbm, wo, send_sem.at[2], wo_recv.at[0], partner)
    loads[8].wait()

    scaling = 1.0 / math.sqrt(head)
    slot_id = lax.broadcasted_iota(jnp.int32, (group, slots), 1)
    stat_lane = lax.broadcasted_iota(jnp.int32, (group, head), 1)
    stat_row = lax.broadcasted_iota(jnp.int32, (group, head), 0)
    stat = jnp.zeros((group, head), F32)
    raw = []
    for c in range(CHUNKS):
        arrived(b_in.at[c], b_recv.at[c])
        total = b_in[c, 0]
        for j in range(1, outer):
            total = total + b_in[c, j]
        for i in range(per):
            b = c * per + i
            q = rotate(total[i, :group], b).astype(BF16)
            key_new = rotate(total[i, group:group + 1], b).astype(BF16).astype(F32)
            value_new = total[i, group + 1:group + 2].astype(BF16).astype(F32)
            s = jnp.dot(q, keys_t[b], preferred_element_type=F32)
            raw.append((q, key_new, value_new, s))
    signal(ready.at[1], partner)
    order = sorted(range(n), key=lambda d: (abs(d - n // 2), d))
    for c in range(CHUNKS):
        accs = []
        for i in range(per):
            b = c * per + i
            q, key_new, value_new, s = raw[b]
            new_score = jnp.sum(q.astype(F32) * key_new, -1, keepdims=True) * scaling
            new_score = jnp.where(owner[b] == me, new_score, -jnp.inf)
            s = jnp.where(slot_id < live[b, me], s * scaling, -jnp.inf)
            top = jnp.maximum(jnp.max(s, -1, keepdims=True), new_score)
            prob = jnp.exp(s - top).astype(BF16)
            new_prob = jnp.exp(new_score - top).astype(BF16).astype(F32)
            count = jnp.sum(prob.astype(F32), -1, keepdims=True) + new_prob
            acc = jnp.dot(prob, vals[b, 0], preferred_element_type=F32)
            accs.append(acc + new_prob * value_new)
            stat = jnp.where(stat_lane == b * group + stat_row, top, stat)
            stat = jnp.where(stat_lane == pairs + b * group + stat_row, count, stat)
        acc_out[c] = jnp.concatenate(accs, 0).astype(BF16)
        if c == 0:
            pl.semaphore_wait(ready.at[1], 1)
        if c == CHUNKS - 1:
            stat_out[...] = jnp.sum(stat, 0, keepdims=True)
            for d in order:
                push(stat_out, stat_in.at[me], send_sem.at[4], stat_recv.at[0], flipped(lax.rem(me + d, n)))
        for d in order:
            push(acc_out.at[c], acc_in.at[c, me], send_sem.at[3], g_recv.at[c], flipped(lax.rem(me + d, n)))

    arrived(stat_in, stat_recv.at[0])
    stats = stat_in[:, 0, :]
    factor = jnp.exp(stats - jnp.max(stats, 0, keepdims=True))
    whole = jnp.sum(factor * pltpu.roll(stats, head - pairs, 1), 0, keepdims=True)
    lane = lax.broadcasted_iota(jnp.int32, stats.shape, 1)
    weight = jnp.where(lane < pairs, factor / whole, 0.0).T
    for c in range(CHUNKS):
        arrived(acc_in.at[c], g_recv.at[c])
        low_row = c * per * group
        high_row = low_row + per * group
        total = weight[low_row:high_row, 0:1] * acc_in[c, 0].astype(F32)
        for j in range(1, n):
            total = total + weight[low_row:high_row, j:j + 1] * acc_in[c, j].astype(F32)
        for i in range(per):
            att_rows[c * per + i] = total[i * group:(i + 1) * group]
    attended = jnp.concatenate([att_rows[:, h, :].astype(BF16) for h in range(group)], -1)

    arrived(wo, wo_recv.at[0])
    kv_buf[other] = jnp.dot(attended, wo[...], preferred_element_type=F32)
    push(kv_buf.at[other], kv_buf.at[other], send_sem.at[5], kv_recv.at[0], partner)
    arrived(kv_buf.at[kv], kv_recv.at[0])
    out[...] = kv_buf[0] + kv_buf[1]
    sent(a_in, send_sem.at[0])
    sent(b_in, send_sem.at[1])
    sent(wo, send_sem.at[2])
    sent(acc_in, send_sem.at[3])
    sent(stat_in, send_sem.at[4])
    sent(kv_buf.at[0], send_sem.at[5])


def local(n, x, wq, wkv, wo, keys, vals, live, owner):
    batch = x.shape[0]
    head = keys.shape[3]
    slots = keys.shape[2]
    rows, qw = wq.shape
    group = qw // head
    cols = wo.shape[1]
    inner = 1
    while inner * inner < n and n % (inner * 2) == 0:
        inner *= 2
    outer = n // inner
    per = batch // CHUNKS
    half = np.float64(ROPE_THETA) ** (-np.arange(0, head, 2, dtype=np.float64) / head)
    freq = jnp.asarray(np.concatenate([half, half]).astype(np.float32)[None, :])
    dma = pltpu.SemaphoreType.DMA
    vmem = pl.BlockSpec(memory_space=pltpu.VMEM)
    hbm = pl.BlockSpec(memory_space=pl.ANY)
    rounds = max(outer.bit_length() - 2, 1)
    return pl.pallas_call(
        functools.partial(kernel, n, inner, outer, group, head),
        out_shape=pltpu.VMEM((batch, cols), F32),
        in_specs=[hbm] * 9,
        out_specs=vmem,
        scratch_shapes=[
            pltpu.SMEM(live.shape, jnp.int32),
            pltpu.SMEM(owner.shape, jnp.int32),
            pltpu.VMEM((1, head), F32),
            pltpu.VMEM((batch, rows), BF16),
            pltpu.VMEM(wq.shape, BF16),
            pltpu.VMEM(wkv.shape, BF16),
            pltpu.VMEM(wo.shape, BF16),
            pltpu.VMEM(keys.shape, BF16),
            pltpu.VMEM((batch, head, slots), BF16),
            pltpu.VMEM(vals.shape, BF16),
            pltpu.VMEM((batch, group + 2, head), F32),
            pltpu.VMEM((CHUNKS, inner, per, group + 2, head), F32),
            pltpu.VMEM((batch, group + 2, head), F32),
            pltpu.VMEM((CHUNKS, outer, per, group + 2, head), F32),
            pltpu.VMEM((CHUNKS, per * group, head), BF16),
            pltpu.VMEM((CHUNKS, n, per * group, head), BF16),
            pltpu.VMEM((1, head), F32),
            pltpu.VMEM((n, 1, head), F32),
            pltpu.VMEM((2, batch, cols), F32),
            pltpu.VMEM((batch, group, head), F32),
            dma((9,)),
            dma((CHUNKS,)), dma((CHUNKS,)), dma((CHUNKS,)),
            dma((6,)),
            dma((1,)), dma((1,)), dma((1,)),
            pltpu.SemaphoreType.REGULAR((2 + rounds,)),
        ],
        compiler_params=pltpu.CompilerParams(collective_id=0, has_side_effects=True),
    )(live, owner, freq, x, wq, wkv, wo, keys, vals).astype(BF16)


def solution(mesh):
    return jax.shard_map(
        functools.partial(local, mesh.shape["seq"]),
        mesh=mesh,
        in_specs=(
            P("dp", None),
            P("seq", "kv"),
            P("seq", "kv"),
            P("kv", "seq"),
            P("dp", "kv", "seq", None),
            P("dp", "kv", "seq", None),
            P("dp", None),
            P("dp"),
        ),
        out_specs=P("dp", "seq"),
        check_vma=False,
    )
```

```python
import functools
import math

import jax
import jax.numpy as jnp
import numpy as np
from jax import lax
from jax.experimental import pallas as pl
from jax.experimental.pallas import tpu as pltpu
from jax.sharding import PartitionSpec as P

ROPE_THETA = 500000.0
F32 = jnp.float32
BF16 = jnp.bfloat16
MESH = pl.DeviceIdType.MESH
CHUNKS = 2
PARTS = 2
PIECES = 4


def kernel(
    n, inner, outer, group, head,
    live_hbm, owner_hbm, freq_hbm, x_hbm, wq_hbm, wkv_hbm, wo_hbm, k_hbm, v_hbm,
    out,
    live, owner, freq, x, wq, wkv, wo, keys, keys_t, vals,
    part, part_new, a_in, a_new, a_sum, sum_new, b_in, b_new,
    acc_out, acc_in, stat_out, stat_in, new_out, new_in, kv_buf, att_rows,
    load_sem, a_recv, b_recv, g_recv, send_sem, pair_recv, ready,
):
    me = lax.axis_index("seq")
    kv = lax.axis_index("kv")
    other = 1 - kv
    batch = x.shape[0]
    rows = wq.shape[0]
    qw = wq.shape[1]
    slots = keys.shape[2]
    per = batch // CHUNKS
    pairs = batch * group
    plane = me // inner
    spot = lax.rem(me, inner)
    partner = {"kv": other}
    steps = [1 << i for i in range(outer.bit_length() - 1)]

    def flipped(j):
        return {"seq": j, "kv": other}

    def across(step):
        return {"seq": (plane + step - 2 * step * lax.rem(plane // step, 2)) * inner + spot}

    def signal(sem, device):
        pl.semaphore_signal(sem, inc=1, device_id=device, device_id_type=MESH)

    def push(src, dst, send, recv, device):
        pltpu.make_async_remote_copy(
            src_ref=src, dst_ref=dst, send_sem=send, recv_sem=recv,
            device_id=device, device_id_type=MESH,
        ).start()

    def arrived(buf, recv):
        pltpu.make_async_remote_copy(
            src_ref=buf, dst_ref=buf, send_sem=send_sem.at[0], recv_sem=recv,
            device_id=partner, device_id_type=MESH,
        ).wait_recv()

    def sent(buf, send):
        pltpu.make_async_remote_copy(
            src_ref=buf, dst_ref=buf, send_sem=send, recv_sem=a_recv.at[0],
            device_id=partner, device_id_type=MESH,
        ).wait_send()

    def in_plane(src, dst, send, recv):
        for d in range(inner - 1, -1, -1):
            push(src, dst, send, recv, flipped(plane * inner + lax.bitwise_xor(spot, d)))

    def over_planes(src, dst, send, recv):
        for d in [outer // 2] + [d for d in range(1, outer) if d != outer // 2] + [0]:
            push(src, dst, send, recv, flipped(lax.rem(plane + d, outer) * inner + spot))

    first = pl.multiple_of(me * rows, rows)
    piece = rows // PIECES
    x_load = pltpu.make_async_copy(x_hbm.at[:, pl.ds(first, rows)], x, load_sem.at[0])
    q_loads = [
        pltpu.make_async_copy(wq_hbm.at[pl.ds(i * piece, piece)], wq.at[pl.ds(i * piece, piece)], load_sem.at[1 + i])
        for i in range(PIECES)
    ]
    later = [(wkv_hbm, wkv), (live_hbm, live), (owner_hbm, owner), (freq_hbm, freq), (k_hbm, keys), (v_hbm, vals)]
    kv_load, live_load, owner_load, freq_load, k_load, v_load = [
        pltpu.make_async_copy(src, dst, load_sem.at[1 + PIECES + i]) for i, (src, dst) in enumerate(later)
    ]
    x_load.start()
    for cp in q_loads:
        cp.start()
    kv_load.start()
    live_load.start()
    owner_load.start()
    freq_load.start()

    barrier = pltpu.get_barrier_semaphore()
    signal(barrier, partner)
    for d in range(1, inner):
        signal(barrier, flipped(plane * inner + lax.rem(spot + d, inner)))
    for step in steps:
        signal(barrier, across(step))

    x_load.wait()
    projected = None
    for i, cp in enumerate(q_loads):
        cp.wait()
        if i == PIECES - 1:
            k_load.start()
            v_load.start()
        term = jnp.dot(x[:, i * piece:(i + 1) * piece], wq[i * piece:(i + 1) * piece, :], preferred_element_type=F32)
        projected = term if projected is None else projected + term
    for h in range(group):
        part[:, h, :] = projected[:, h * head:(h + 1) * head]
    pl.semaphore_wait(barrier, inner + len(steps))

    for c in range(CHUNKS):
        in_plane(part.at[pl.ds(c * per, per)], a_in.at[c, spot], send_sem.at[0], a_recv.at[c])

    kv_load.wait()
    both = jnp.dot(x[...], wkv[...], preferred_element_type=F32)
    part_new[0] = both[:, :head]
    part_new[1] = both[:, head:]
    in_plane(part_new, a_new.at[spot], send_sem.at[0], a_recv.at[CHUNKS])

    live_load.wait()
    owner_load.wait()
    freq_load.wait()
    row_id = lax.broadcasted_iota(jnp.int32, (batch, head), 0)
    lane_id = lax.broadcasted_iota(jnp.int32, (batch, head), 1)
    position = jnp.zeros((batch, head), jnp.int32)
    for b in range(batch):
        own = owner[b]
        position = jnp.where(row_id == b, own * slots + live[b, own], position)
    angle = position.astype(F32) * freq[...]
    cosine = jnp.cos(angle)
    sine = jnp.sin(angle)
    sine = jnp.where(lane_id < head // 2, -sine, sine)

    for i in range(max(len(steps) - 1, 1)):
        for step in steps:
            signal(ready.at[2 + i], across(step))
        if i == 0:
            k_load.wait()
            for b in range(batch):
                keys_t[b] = keys[b, 0].T
        pl.semaphore_wait(ready.at[2 + i], len(steps))
    signal(ready.at[0], partner)
    pl.semaphore_wait(ready.at[0], 1)

    for c in range(CHUNKS):
        arrived(a_in.at[c], a_recv.at[c])
        total = a_in[c, 0]
        for j in range(1, inner):
            total = total + a_in[c, j]
        a_sum[c * per:(c + 1) * per] = total
        over_planes(a_sum.at[pl.ds(c * per, per)], b_in.at[c, plane], send_sem.at[0], b_recv.at[c])
    arrived(a_new, a_recv.at[CHUNKS])
    total = a_new[0]
    for j in range(1, inner):
        total = total + a_new[j]
    sum_new[...] = total
    over_planes(sum_new, b_new.at[plane], send_sem.at[0], b_recv.at[CHUNKS])
    push(wo_hbm, wo, send_sem.at[0], pair_recv.at[0], partner)
    v_load.wait()

    scaling = 1.0 / math.sqrt(head)
    slot_id = lax.broadcasted_iota(jnp.int32, (group, slots), 1)
    stat_lane = lax.broadcasted_iota(jnp.int32, (group, head), 1)
    stat_row = lax.broadcasted_iota(jnp.int32, (group, head), 0)
    stat = jnp.zeros((group, head), F32)
    queries = []
    order = [
        lax.rem(plane + dz, outer) * inner + lax.bitwise_xor(spot, ds)
        for ds in sorted(range(inner), key=lambda v: (v % 2 == 0, -v))
        for dz in sorted(range(outer), key=lambda v: -min(v, outer - v))
    ]
    scores = []
    for c in range(CHUNKS):
        arrived(b_in.at[c], b_recv.at[c])
        if c == 0:
            signal(ready.at[1], partner)
        total = b_in[c, 0]
        for j in range(1, outer):
            total = total + b_in[c, j]
        for i in range(per):
            b = c * per + i
            q = total[i] * cosine[b:b + 1] + pltpu.roll(total[i], head // 2, 1) * sine[b:b + 1]
            q = q.astype(BF16)
            queries.append(q)
            scores.append(jnp.dot(q, keys_t[b], preferred_element_type=F32))
    few = batch // PARTS
    for c in range(PARTS):
        accs = []
        for b in range(c * few, c * few + few):
            s = jnp.where(slot_id < live[b, me], scores[b] * scaling, -jnp.inf)
            top = jnp.max(s, -1, keepdims=True)
            prob = jnp.exp(s - top).astype(BF16)
            count = jnp.sum(prob.astype(F32), -1, keepdims=True)
            accs.append(jnp.dot(prob, vals[b, 0], preferred_element_type=F32))
            stat = jnp.where(stat_lane == b * group + stat_row, top, stat)
            stat = jnp.where(stat_lane == pairs + b * group + stat_row, count, stat)
        acc_out[c] = jnp.concatenate(accs, 0).astype(BF16)
        if c == 0:
            pl.semaphore_wait(ready.at[1], 1)
        if c == PARTS - 1:
            stat_out[...] = jnp.sum(stat, 0, keepdims=True)
            for j in order:
                push(stat_out, stat_in.at[me], send_sem.at[0], pair_recv.at[3], flipped(j))
        for j in order:
            push(acc_out.at[c], acc_in.at[c, me], send_sem.at[0], g_recv.at[c], flipped(j))

    arrived(b_new, b_recv.at[CHUNKS])
    total = b_new[0]
    for j in range(1, outer):
        total = total + b_new[j]
    key_new = total[0] * cosine + pltpu.roll(total[0], head // 2, 1) * sine
    key_new = key_new.astype(BF16).astype(F32)
    fresh = jnp.where(stat_lane >= pairs, 1.0 / group, 0.0)
    for b in range(batch):
        score = jnp.sum(queries[b].astype(F32) * key_new[b:b + 1], -1, keepdims=True) * scaling
        fresh = jnp.where(stat_lane == b * group + stat_row, score, fresh)
    new_out[:batch] = total[1].astype(BF16).astype(F32)
    new_out[batch:batch + 1] = jnp.sum(fresh, 0, keepdims=True)
    push(new_out, new_in, send_sem.at[0], pair_recv.at[1], partner)

    arrived(stat_in, pair_recv.at[3])
    arrived(new_in, pair_recv.at[1])
    stats = stat_in[:, 0, :]
    newest = new_in[batch:batch + 1]
    top = jnp.maximum(jnp.max(stats, 0, keepdims=True), newest)
    factor = jnp.exp(stats - top)
    fresh = jnp.exp(newest - top)
    whole = jnp.sum(factor * pltpu.roll(stats, head - pairs, 1), 0, keepdims=True) + fresh
    lane = lax.broadcasted_iota(jnp.int32, stats.shape, 1)
    weight = jnp.where(lane < pairs, factor / whole, 0.0).T
    fresh = jnp.where(lane[:1] < pairs, fresh / whole, 0.0)
    fresh = jnp.broadcast_to(fresh, (group, head)).T
    for c in range(PARTS):
        arrived(acc_in.at[c], g_recv.at[c])
        low_row = c * few * group
        high_row = low_row + few * group
        total = weight[low_row:high_row, 0:1] * acc_in[c, 0].astype(F32)
        for j in range(1, n):
            total = total + weight[low_row:high_row, j:j + 1] * acc_in[c, j].astype(F32)
        for i in range(few):
            b = c * few + i
            own = fresh[b * group:(b + 1) * group, 0:1] * new_in[b:b + 1]
            att_rows[b] = total[i * group:(i + 1) * group] + own
    attended = jnp.concatenate([att_rows[:, h, :].astype(BF16) for h in range(group)], -1)

    arrived(wo, pair_recv.at[0])
    kv_buf[other] = jnp.dot(attended, wo[...], preferred_element_type=F32)
    push(kv_buf.at[other], kv_buf.at[other], send_sem.at[0], pair_recv.at[2], partner)
    arrived(kv_buf.at[kv], pair_recv.at[2])
    out[...] = kv_buf[0] + kv_buf[1]
    sent(a_in, send_sem.at[0])
    sent(b_in, send_sem.at[0])
    sent(a_new, send_sem.at[0])
    sent(b_new, send_sem.at[0])
    sent(wo, send_sem.at[0])
    sent(acc_in, send_sem.at[0])
    sent(stat_in, send_sem.at[0])
    sent(new_in, send_sem.at[0])
    sent(kv_buf.at[0], send_sem.at[0])


def local(n, x, wq, wkv, wo, keys, vals, live, owner):
    batch = x.shape[0]
    head = keys.shape[3]
    slots = keys.shape[2]
    rows, qw = wq.shape
    group = qw // head
    cols = wo.shape[1]
    inner = 1
    while inner * inner < n and n % (inner * 2) == 0:
        inner *= 2
    outer = n // inner
    per = batch // CHUNKS
    half = np.float64(ROPE_THETA) ** (-np.arange(0, head, 2, dtype=np.float64) / head)
    freq = jnp.asarray(np.concatenate([half, half]).astype(np.float32)[None, :])
    dma = pltpu.SemaphoreType.DMA
    vmem = pl.BlockSpec(memory_space=pltpu.VMEM)
    hbm = pl.BlockSpec(memory_space=pl.ANY)
    rounds = max(outer.bit_length() - 2, 1)
    return pl.pallas_call(
        functools.partial(kernel, n, inner, outer, group, head),
        out_shape=pltpu.VMEM((batch, cols), F32),
        in_specs=[hbm] * 9,
        out_specs=vmem,
        scratch_shapes=[
            pltpu.SMEM(live.shape, jnp.int32),
            pltpu.SMEM(owner.shape, jnp.int32),
            pltpu.VMEM((1, head), F32),
            pltpu.VMEM((batch, rows), BF16),
            pltpu.VMEM(wq.shape, BF16),
            pltpu.VMEM(wkv.shape, BF16),
            pltpu.VMEM(wo.shape, BF16),
            pltpu.VMEM(keys.shape, BF16),
            pltpu.VMEM((batch, head, slots), BF16),
            pltpu.VMEM(vals.shape, BF16),
            pltpu.VMEM((batch, group, head), F32),
            pltpu.VMEM((2, batch, head), F32),
            pltpu.VMEM((CHUNKS, inner, per, group, head), F32),
            pltpu.VMEM((inner, 2, batch, head), F32),
            pltpu.VMEM((batch, group, head), F32),
            pltpu.VMEM((2, batch, head), F32),
            pltpu.VMEM((CHUNKS, outer, per, group, head), F32),
            pltpu.VMEM((outer, 2, batch, head), F32),
            pltpu.VMEM((PARTS, batch // PARTS * group, head), BF16),
            pltpu.VMEM((PARTS, n, batch // PARTS * group, head), BF16),
            pltpu.VMEM((1, head), F32),
            pltpu.VMEM((n, 1, head), F32),
            pltpu.VMEM((batch + 1, head), F32),
            pltpu.VMEM((batch + 1, head), F32),
            pltpu.VMEM((2, batch, cols), F32),
            pltpu.VMEM((batch, group, head), F32),
            dma((7 + PIECES,)),
            dma((CHUNKS + 1,)), dma((CHUNKS + 1,)), dma((PARTS,)),
            dma((1,)),
            dma((4,)),
            pltpu.SemaphoreType.REGULAR((2 + rounds,)),
        ],
        compiler_params=pltpu.CompilerParams(collective_id=0, has_side_effects=True),
    )(live, owner, freq, x, wq, wkv, wo, keys, vals).astype(BF16)


def solution(mesh):
    return jax.shard_map(
        functools.partial(local, mesh.shape["seq"]),
        mesh=mesh,
        in_specs=(
            P("dp", None),
            P("seq", "kv"),
            P("seq", "kv"),
            P("kv", "seq"),
            P("dp", "kv", "seq", None),
            P("dp", "kv", "seq", None),
            P("dp", None),
            P("dp"),
        ),
        out_specs=P("dp", "seq"),
        check_vma=False,
    )
```

```python
import functools
import math

import jax
import jax.numpy as jnp
import numpy as np
from jax import lax
from jax.experimental import pallas as pl
from jax.experimental.pallas import tpu as pltpu
from jax.sharding import PartitionSpec as P

ROPE_THETA = 500000.0
F32 = jnp.float32
BF16 = jnp.bfloat16
MESH = pl.DeviceIdType.MESH
CHUNKS = 2
PARTS = 1
PIECES = 4


def kernel(
    n, inner, outer, group, head,
    live_hbm, owner_hbm, freq_hbm, x_hbm, wq_hbm, wkv_hbm, wo_hbm, k_hbm, v_hbm,
    out,
    live, owner, freq, x, wq, wkv, wo, keys, keys_t, vals,
    part, part_new, a_in, a_new, a_sum, sum_new, b_in, b_new,
    acc_out, acc_in, stat_out, stat_in, new_out, new_in, kv_buf, att_rows,
    load_sem, a_recv, b_recv, g_recv, send_sem, pair_recv, ready,
):
    me = lax.axis_index("seq")
    kv = lax.axis_index("kv")
    other = 1 - kv
    batch = x.shape[0]
    rows = wq.shape[0]
    qw = wq.shape[1]
    slots = keys.shape[2]
    per = batch // CHUNKS
    pairs = batch * group
    plane = me // inner
    spot = lax.rem(me, inner)
    partner = {"kv": other}
    steps = [1 << i for i in range(outer.bit_length() - 1)]

    def flipped(j):
        return {"seq": j, "kv": other}

    def across(step):
        return {"seq": (plane + step - 2 * step * lax.rem(plane // step, 2)) * inner + spot}

    def signal(sem, device):
        pl.semaphore_signal(sem, inc=1, device_id=device, device_id_type=MESH)

    def push(src, dst, send, recv, device):
        pltpu.make_async_remote_copy(
            src_ref=src, dst_ref=dst, send_sem=send, recv_sem=recv,
            device_id=device, device_id_type=MESH,
        ).start()

    def arrived(buf, recv):
        pltpu.make_async_remote_copy(
            src_ref=buf, dst_ref=buf, send_sem=send_sem.at[0], recv_sem=recv,
            device_id=partner, device_id_type=MESH,
        ).wait_recv()

    def sent(buf, send):
        pltpu.make_async_remote_copy(
            src_ref=buf, dst_ref=buf, send_sem=send, recv_sem=a_recv.at[0],
            device_id=partner, device_id_type=MESH,
        ).wait_send()

    def in_plane(src, dst, send, recv):
        for d in range(inner - 1, -1, -1):
            push(src, dst, send, recv, flipped(plane * inner + lax.bitwise_xor(spot, d)))

    def over_planes(src, dst, send, recv):
        for rank in ranks:
            push(src, dst, send, recv, flipped(rank * inner + spot))

    up = plane // (outer // 2)
    ranks = [up * k + (1 - up) * (outer - 1 - k) for k in range(outer)]
    order = [rank * inner + lax.bitwise_xor(spot, ds) for rank in ranks for ds in range(inner - 1, -1, -1)]
    first = pl.multiple_of(me * rows, rows)
    piece = rows // PIECES
    x_load = pltpu.make_async_copy(x_hbm.at[:, pl.ds(first, rows)], x, load_sem.at[0])
    q_loads = [
        pltpu.make_async_copy(wq_hbm.at[pl.ds(i * piece, piece)], wq.at[pl.ds(i * piece, piece)], load_sem.at[1 + i])
        for i in range(PIECES)
    ]
    later = [(wkv_hbm, wkv), (live_hbm, live), (owner_hbm, owner), (freq_hbm, freq), (k_hbm, keys), (v_hbm, vals)]
    kv_load, live_load, owner_load, freq_load, k_load, v_load = [
        pltpu.make_async_copy(src, dst, load_sem.at[1 + PIECES + i]) for i, (src, dst) in enumerate(later)
    ]
    x_load.start()
    for cp in q_loads:
        cp.start()
    kv_load.start()
    live_load.start()
    owner_load.start()
    freq_load.start()

    barrier = pltpu.get_barrier_semaphore()
    signal(barrier, partner)
    for d in range(1, inner):
        signal(barrier, flipped(plane * inner + lax.rem(spot + d, inner)))
    for step in steps:
        signal(barrier, across(step))

    x_load.wait()
    projected = None
    for i, cp in enumerate(q_loads):
        cp.wait()
        if i == PIECES - 1:
            k_load.start()
            v_load.start()
        term = jnp.dot(x[:, i * piece:(i + 1) * piece], wq[i * piece:(i + 1) * piece, :], preferred_element_type=F32)
        projected = term if projected is None else projected + term
    for h in range(group):
        part[:, h, :] = projected[:, h * head:(h + 1) * head]
    pl.semaphore_wait(barrier, inner + len(steps))
    for step in steps:
        signal(ready.at[2], across(step))

    for c in range(CHUNKS):
        in_plane(part.at[pl.ds(c * per, per)], a_in.at[c, spot], send_sem.at[0], a_recv.at[c])

    kv_load.wait()
    both = jnp.dot(x[...], wkv[...], preferred_element_type=F32)
    part_new[0] = both[:, :head]
    part_new[1] = both[:, head:]
    in_plane(part_new, a_new.at[spot], send_sem.at[0], a_recv.at[CHUNKS])

    live_load.wait()
    owner_load.wait()
    freq_load.wait()
    row_id = lax.broadcasted_iota(jnp.int32, (batch, head), 0)
    lane_id = lax.broadcasted_iota(jnp.int32, (batch, head), 1)
    position = jnp.zeros((batch, head), jnp.int32)
    for b in range(batch):
        own = owner[b]
        position = jnp.where(row_id == b, own * slots + live[b, own], position)
    angle = position.astype(F32) * freq[...]
    cosine = jnp.cos(angle)
    sine = jnp.sin(angle)
    sine = jnp.where(lane_id < head // 2, -sine, sine)

    k_load.wait()
    for b in range(batch):
        keys_t[b] = keys[b, 0].T
    pl.semaphore_wait(ready.at[2], len(steps))
    for i in range(1, len(steps) - 1):
        for step in steps:
            signal(ready.at[2 + i], across(step))
        pl.semaphore_wait(ready.at[2 + i], len(steps))
    signal(ready.at[0], partner)
    pl.semaphore_wait(ready.at[0], 1)

    for c in range(CHUNKS):
        arrived(a_in.at[c], a_recv.at[c])
        total = a_in[c, 0]
        for j in range(1, inner):
            total = total + a_in[c, j]
        a_sum[c * per:(c + 1) * per] = total
        over_planes(a_sum.at[pl.ds(c * per, per)], b_in.at[c, plane], send_sem.at[0], b_recv.at[c])
    arrived(a_new, a_recv.at[CHUNKS])
    total = a_new[0]
    for j in range(1, inner):
        total = total + a_new[j]
    sum_new[...] = total
    over_planes(sum_new, b_new.at[plane], send_sem.at[0], b_recv.at[CHUNKS])
    push(wo_hbm, wo, send_sem.at[0], pair_recv.at[0], partner)
    v_load.wait()

    scaling = 1.0 / math.sqrt(head)
    slot_id = lax.broadcasted_iota(jnp.int32, (group, slots), 1)
    stat_lane = lax.broadcasted_iota(jnp.int32, (group, head), 1)
    stat_row = lax.broadcasted_iota(jnp.int32, (group, head), 0)
    stat = jnp.zeros((group, head), F32)
    queries = []
    scores = []
    for c in range(CHUNKS):
        arrived(b_in.at[c], b_recv.at[c])
        if c == 0:
            signal(ready.at[1], partner)
        total = b_in[c, 0]
        for j in range(1, outer):
            total = total + b_in[c, j]
        for i in range(per):
            b = c * per + i
            q = total[i] * cosine[b:b + 1] + pltpu.roll(total[i], head // 2, 1) * sine[b:b + 1]
            q = q.astype(BF16)
            queries.append(q)
            scores.append(jnp.dot(q, keys_t[b], preferred_element_type=F32))
    few = batch // PARTS
    for c in range(PARTS):
        accs = []
        for b in range(c * few, c * few + few):
            s = jnp.where(slot_id < live[b, me], scores[b] * scaling, -jnp.inf)
            top = jnp.max(s, -1, keepdims=True)
            prob = jnp.exp(s - top).astype(BF16)
            count = jnp.sum(prob.astype(F32), -1, keepdims=True)
            accs.append(jnp.dot(prob, vals[b, 0], preferred_element_type=F32))
            stat = jnp.where(stat_lane == b * group + stat_row, top, stat)
            stat = jnp.where(stat_lane == pairs + b * group + stat_row, count, stat)
        acc_out[c] = jnp.concatenate(accs, 0).astype(BF16)
        if c == 0:
            pl.semaphore_wait(ready.at[1], 1)
        if c == PARTS - 1:
            stat_out[...] = jnp.sum(stat, 0, keepdims=True)
            for j in order:
                push(stat_out, stat_in.at[me], send_sem.at[0], pair_recv.at[3], flipped(j))
        for j in order:
            push(acc_out.at[c], acc_in.at[c, me], send_sem.at[0], g_recv.at[c], flipped(j))

    arrived(b_new, b_recv.at[CHUNKS])
    total = b_new[0]
    for j in range(1, outer):
        total = total + b_new[j]
    key_new = total[0] * cosine + pltpu.roll(total[0], head // 2, 1) * sine
    key_new = key_new.astype(BF16).astype(F32)
    fresh = jnp.where(stat_lane >= pairs, 1.0 / group, 0.0)
    for b in range(batch):
        score = jnp.sum(queries[b].astype(F32) * key_new[b:b + 1], -1, keepdims=True) * scaling
        fresh = jnp.where(stat_lane == b * group + stat_row, score, fresh)
    new_out[:batch] = total[1].astype(BF16).astype(F32)
    new_out[batch:batch + 1] = jnp.sum(fresh, 0, keepdims=True)
    push(new_out, new_in, send_sem.at[0], pair_recv.at[1], partner)

    arrived(stat_in, pair_recv.at[3])
    arrived(new_in, pair_recv.at[1])
    stats = stat_in[:, 0, :]
    newest = new_in[batch:batch + 1]
    top = jnp.maximum(jnp.max(stats, 0, keepdims=True), newest)
    factor = jnp.exp(stats - top)
    fresh = jnp.exp(newest - top)
    whole = jnp.sum(factor * pltpu.roll(stats, head - pairs, 1), 0, keepdims=True) + fresh
    lane = lax.broadcasted_iota(jnp.int32, stats.shape, 1)
    weight = jnp.where(lane < pairs, factor / whole, 0.0).T
    fresh = jnp.where(lane[:1] < pairs, fresh / whole, 0.0)
    fresh = jnp.broadcast_to(fresh, (group, head)).T
    for c in range(PARTS):
        arrived(acc_in.at[c], g_recv.at[c])
        low_row = c * few * group
        high_row = low_row + few * group
        total = weight[low_row:high_row, 0:1] * acc_in[c, 0].astype(F32)
        for j in range(1, n):
            total = total + weight[low_row:high_row, j:j + 1] * acc_in[c, j].astype(F32)
        for i in range(few):
            b = c * few + i
            own = fresh[b * group:(b + 1) * group, 0:1] * new_in[b:b + 1]
            att_rows[b] = total[i * group:(i + 1) * group] + own
    attended = jnp.concatenate([att_rows[:, h, :].astype(BF16) for h in range(group)], -1)

    arrived(wo, pair_recv.at[0])
    kv_buf[other] = jnp.dot(attended, wo[...], preferred_element_type=F32)
    push(kv_buf.at[other], kv_buf.at[other], send_sem.at[0], pair_recv.at[2], partner)
    arrived(kv_buf.at[kv], pair_recv.at[2])
    out[...] = kv_buf[0] + kv_buf[1]
    sent(a_in, send_sem.at[0])
    sent(b_in, send_sem.at[0])
    sent(a_new, send_sem.at[0])
    sent(b_new, send_sem.at[0])
    sent(wo, send_sem.at[0])
    sent(acc_in, send_sem.at[0])
    sent(stat_in, send_sem.at[0])
    sent(new_in, send_sem.at[0])
    sent(kv_buf.at[0], send_sem.at[0])


def local(n, x, wq, wkv, wo, keys, vals, live, owner):
    batch = x.shape[0]
    head = keys.shape[3]
    slots = keys.shape[2]
    rows, qw = wq.shape
    group = qw // head
    cols = wo.shape[1]
    inner = 1
    while inner * inner < n and n % (inner * 2) == 0:
        inner *= 2
    outer = n // inner
    per = batch // CHUNKS
    half = np.float64(ROPE_THETA) ** (-np.arange(0, head, 2, dtype=np.float64) / head)
    freq = jnp.asarray(np.concatenate([half, half]).astype(np.float32)[None, :])
    dma = pltpu.SemaphoreType.DMA
    vmem = pl.BlockSpec(memory_space=pltpu.VMEM)
    hbm = pl.BlockSpec(memory_space=pl.ANY)
    rounds = max(outer.bit_length() - 2, 1)
    return pl.pallas_call(
        functools.partial(kernel, n, inner, outer, group, head),
        out_shape=pltpu.VMEM((batch, cols), F32),
        in_specs=[hbm] * 9,
        out_specs=vmem,
        scratch_shapes=[
            pltpu.SMEM(live.shape, jnp.int32),
            pltpu.SMEM(owner.shape, jnp.int32),
            pltpu.VMEM((1, head), F32),
            pltpu.VMEM((batch, rows), BF16),
            pltpu.VMEM(wq.shape, BF16),
            pltpu.VMEM(wkv.shape, BF16),
            pltpu.VMEM(wo.shape, BF16),
            pltpu.VMEM(keys.shape, BF16),
            pltpu.VMEM((batch, head, slots), BF16),
            pltpu.VMEM(vals.shape, BF16),
            pltpu.VMEM((batch, group, head), F32),
            pltpu.VMEM((2, batch, head), F32),
            pltpu.VMEM((CHUNKS, inner, per, group, head), F32),
            pltpu.VMEM((inner, 2, batch, head), F32),
            pltpu.VMEM((batch, group, head), F32),
            pltpu.VMEM((2, batch, head), F32),
            pltpu.VMEM((CHUNKS, outer, per, group, head), F32),
            pltpu.VMEM((outer, 2, batch, head), F32),
            pltpu.VMEM((PARTS, batch // PARTS * group, head), BF16),
            pltpu.VMEM((PARTS, n, batch // PARTS * group, head), BF16),
            pltpu.VMEM((1, head), F32),
            pltpu.VMEM((n, 1, head), F32),
            pltpu.VMEM((batch + 1, head), F32),
            pltpu.VMEM((batch + 1, head), F32),
            pltpu.VMEM((2, batch, cols), F32),
            pltpu.VMEM((batch, group, head), F32),
            dma((7 + PIECES,)),
            dma((CHUNKS + 1,)), dma((CHUNKS + 1,)), dma((PARTS,)),
            dma((1,)),
            dma((4,)),
            pltpu.SemaphoreType.REGULAR((2 + rounds,)),
        ],
        compiler_params=pltpu.CompilerParams(collective_id=0, has_side_effects=True),
    )(live, owner, freq, x, wq, wkv, wo, keys, vals).astype(BF16)


def solution(mesh):
    return jax.shard_map(
        functools.partial(local, mesh.shape["seq"]),
        mesh=mesh,
        in_specs=(
            P("dp", None),
            P("seq", "kv"),
            P("seq", "kv"),
            P("kv", "seq"),
            P("dp", "kv", "seq", None),
            P("dp", "kv", "seq", None),
            P("dp", None),
            P("dp"),
        ),
        out_specs=P("dp", "seq"),
        check_vma=False,
    )
```

```python
import functools
import math

import jax
import jax.numpy as jnp
import numpy as np
from jax import lax
from jax.experimental import pallas as pl
from jax.experimental.pallas import tpu as pltpu
from jax.sharding import PartitionSpec as P

ROPE_THETA = 500000.0
F32 = jnp.float32
BF16 = jnp.bfloat16
MESH = pl.DeviceIdType.MESH
CHUNKS = 2
PIECES = 4


def kernel(
    n, inner, outer, group, head,
    live_hbm, owner_hbm, freq_hbm, x_hbm, wq_hbm, wkv_hbm, wo_hbm, k_hbm, v_hbm,
    out,
    live, owner, freq, x, wq, wkv, wo, keys, keys_t, vals,
    part, part_new, a_in, a_new, a_sum, sum_new, b_in, b_new,
    acc_out, acc_in, stat_out, stat_in, new_out, new_in, kv_buf, att_rows,
    load_sem, a_recv, b_recv, g_recv, send_sem, pair_recv, ready,
):
    me = lax.axis_index("seq")
    kv = lax.axis_index("kv")
    other = 1 - kv
    batch = x.shape[0]
    rows = wq.shape[0]
    qw = wq.shape[1]
    slots = keys.shape[2]
    per = batch // CHUNKS
    pairs = batch * group
    plane = me // inner
    spot = lax.rem(me, inner)
    partner = {"kv": other}
    steps = [1 << i for i in range(outer.bit_length() - 1)]

    def flipped(j):
        return {"seq": j, "kv": other}

    def across(step):
        return {"seq": (plane + step - 2 * step * lax.rem(plane // step, 2)) * inner + spot}

    def signal(sem, device):
        pl.semaphore_signal(sem, inc=1, device_id=device, device_id_type=MESH)

    def push(src, dst, send, recv, device):
        pltpu.make_async_remote_copy(
            src_ref=src, dst_ref=dst, send_sem=send, recv_sem=recv,
            device_id=device, device_id_type=MESH,
        ).start()

    def arrived(buf, recv):
        pltpu.make_async_remote_copy(
            src_ref=buf, dst_ref=buf, send_sem=send_sem.at[0], recv_sem=recv,
            device_id=partner, device_id_type=MESH,
        ).wait_recv()

    def sent(buf, send):
        pltpu.make_async_remote_copy(
            src_ref=buf, dst_ref=buf, send_sem=send, recv_sem=a_recv.at[0],
            device_id=partner, device_id_type=MESH,
        ).wait_send()

    def in_plane(src, dst, send, recv):
        for d in range(inner - 1, -1, -1):
            push(src, dst, send, recv, flipped(plane * inner + lax.bitwise_xor(spot, d)))

    def over_planes(src, dst, send, recv):
        for rank in ranks:
            push(src, dst, send, recv, flipped(rank * inner + spot))

    up = plane // (outer // 2)
    ranks = [up * k + (1 - up) * (outer - 1 - k) for k in range(outer)]
    order = [rank * inner + lax.bitwise_xor(spot, ds) for rank in ranks for ds in range(inner - 1, -1, -1)]
    first = pl.multiple_of(me * rows, rows)
    piece = rows // PIECES
    x_load = pltpu.make_async_copy(x_hbm.at[:, pl.ds(first, rows)], x, load_sem.at[0])
    q_loads = [
        pltpu.make_async_copy(wq_hbm.at[pl.ds(i * piece, piece)], wq.at[pl.ds(i * piece, piece)], load_sem.at[1 + i])
        for i in range(PIECES)
    ]
    kv_load = pltpu.make_async_copy(wkv_hbm, wkv, load_sem.at[1 + PIECES])
    later = [(live_hbm, live), (owner_hbm, owner), (freq_hbm, freq), (k_hbm, keys), (v_hbm, vals)]
    live_load, owner_load, freq_load, k_load, v_load = [
        pltpu.make_async_copy(src, dst, load_sem.at[i]) for i, (src, dst) in enumerate(later)
    ]
    x_load.start()
    for cp in q_loads:
        cp.start()
    kv_load.start()

    barrier = pltpu.get_barrier_semaphore()
    signal(barrier, partner)
    for d in range(1, inner):
        signal(barrier, flipped(plane * inner + lax.rem(spot + d, inner)))
    for step in steps:
        signal(barrier, across(step))

    x_load.wait()
    live_load.start()
    projected = None
    for i, cp in enumerate(q_loads):
        cp.wait()
        if i == 0:
            owner_load.start()
        if i == 1:
            freq_load.start()
        if i == PIECES - 1:
            k_load.start()
            v_load.start()
        term = jnp.dot(x[:, i * piece:(i + 1) * piece], wq[i * piece:(i + 1) * piece, :], preferred_element_type=F32)
        projected = term if projected is None else projected + term
    for h in range(group):
        part[:, h, :] = projected[:, h * head:(h + 1) * head]
    pl.semaphore_wait(barrier, inner + len(steps))
    for step in steps:
        signal(ready.at[2], across(step))

    for c in range(CHUNKS):
        in_plane(part.at[pl.ds(c * per, per)], a_in.at[c, spot], send_sem.at[0], a_recv.at[c])

    kv_load.wait()
    both = jnp.dot(x[...], wkv[...], preferred_element_type=F32)
    part_new[0] = both[:, :head]
    part_new[1] = both[:, head:]
    in_plane(part_new, a_new.at[spot], send_sem.at[0], a_recv.at[CHUNKS])

    live_load.wait()
    owner_load.wait()
    freq_load.wait()
    row_id = lax.broadcasted_iota(jnp.int32, (batch, head), 0)
    lane_id = lax.broadcasted_iota(jnp.int32, (batch, head), 1)
    position = jnp.zeros((batch, head), jnp.int32)
    for b in range(batch):
        own = owner[b]
        position = jnp.where(row_id == b, own * slots + live[b, own], position)
    angle = position.astype(F32) * freq[...]
    cosine = jnp.cos(angle)
    sine = jnp.sin(angle)
    sine = jnp.where(lane_id < head // 2, -sine, sine)

    k_load.wait()
    for b in range(batch):
        keys_t[b] = keys[b, 0].T
    pl.semaphore_wait(ready.at[2], len(steps))
    for i in range(1, len(steps) - 1):
        for step in steps:
            signal(ready.at[2 + i], across(step))
        pl.semaphore_wait(ready.at[2 + i], len(steps))
    signal(ready.at[0], partner)
    pl.semaphore_wait(ready.at[0], 1)

    for c in range(CHUNKS):
        arrived(a_in.at[c], a_recv.at[c])
        total = a_in[c, 0]
        for j in range(1, inner):
            total = total + a_in[c, j]
        a_sum[c * per:(c + 1) * per] = total
        over_planes(a_sum.at[pl.ds(c * per, per)], b_in.at[c, plane], send_sem.at[0], b_recv.at[c])
    arrived(a_new, a_recv.at[CHUNKS])
    total = a_new[0]
    for j in range(1, inner):
        total = total + a_new[j]
    sum_new[...] = total
    over_planes(sum_new, b_new.at[plane], send_sem.at[0], b_recv.at[CHUNKS])
    push(wo_hbm, wo, send_sem.at[0], pair_recv.at[0], partner)
    v_load.wait()

    scaling = 1.0 / math.sqrt(head)
    slot_id = lax.broadcasted_iota(jnp.int32, (group, slots), 1)
    stat_lane = lax.broadcasted_iota(jnp.int32, (group, head), 1)
    stat_row = lax.broadcasted_iota(jnp.int32, (group, head), 0)
    stat = jnp.zeros((group, head), F32)
    queries = []
    scores = []
    for c in range(CHUNKS):
        arrived(b_in.at[c], b_recv.at[c])
        if c == 0:
            signal(ready.at[1], partner)
        total = b_in[c, 0]
        for j in range(1, outer):
            total = total + b_in[c, j]
        for i in range(per):
            b = c * per + i
            q = total[i] * cosine[b:b + 1] + pltpu.roll(total[i], head // 2, 1) * sine[b:b + 1]
            q = q.astype(BF16)
            queries.append(q)
            scores.append(jnp.dot(q, keys_t[b], preferred_element_type=F32))
    accs = []
    for b in range(batch):
        s = jnp.where(slot_id < live[b, me], scores[b] * scaling, -jnp.inf)
        top = jnp.max(s, -1, keepdims=True)
        prob = jnp.exp(s - top).astype(BF16)
        count = jnp.sum(prob.astype(F32), -1, keepdims=True)
        accs.append(jnp.dot(prob, vals[b, 0], preferred_element_type=F32))
        stat = jnp.where(stat_lane == b * group + stat_row, top, stat)
        stat = jnp.where(stat_lane == pairs + b * group + stat_row, count, stat)
    acc_out[...] = jnp.concatenate(accs, 0).astype(BF16)
    stat_out[...] = jnp.sum(stat, 0, keepdims=True)
    pl.semaphore_wait(ready.at[1], 1)
    for side in range(2):
        peers = order[side * n // 2:(side + 1) * n // 2]
        for j in peers:
            push(stat_out, stat_in.at[me], send_sem.at[0], pair_recv.at[3], flipped(j))
        for j in peers:
            push(acc_out, acc_in.at[me], send_sem.at[0], g_recv.at[up], flipped(j))

    arrived(b_new, b_recv.at[CHUNKS])
    total = b_new[0]
    for j in range(1, outer):
        total = total + b_new[j]
    key_new = total[0] * cosine + pltpu.roll(total[0], head // 2, 1) * sine
    key_new = key_new.astype(BF16).astype(F32)
    fresh = jnp.where(stat_lane >= pairs, 1.0 / group, 0.0)
    for b in range(batch):
        score = jnp.sum(queries[b].astype(F32) * key_new[b:b + 1], -1, keepdims=True) * scaling
        fresh = jnp.where(stat_lane == b * group + stat_row, score, fresh)
    new_out[:batch] = total[1].astype(BF16).astype(F32)
    new_out[batch:batch + 1] = jnp.sum(fresh, 0, keepdims=True)
    push(new_out, new_in, send_sem.at[0], pair_recv.at[1], partner)

    arrived(stat_in, pair_recv.at[3])
    arrived(new_in, pair_recv.at[1])
    near = pl.multiple_of(up * (n // 2), n // 2)
    far = pl.multiple_of((1 - up) * (n // 2), n // 2)
    stats = jnp.concatenate([stat_in[pl.ds(near, n // 2), 0, :], stat_in[pl.ds(far, n // 2), 0, :]], 0)
    newest = new_in[batch:batch + 1]
    top = jnp.maximum(jnp.max(stats, 0, keepdims=True), newest)
    factor = jnp.exp(stats - top)
    fresh = jnp.exp(newest - top)
    whole = jnp.sum(factor * pltpu.roll(stats, head - pairs, 1), 0, keepdims=True) + fresh
    lane = lax.broadcasted_iota(jnp.int32, stats.shape, 1)
    weight = jnp.where(lane < pairs, factor / whole, 0.0).T
    fresh = jnp.where(lane[:1] < pairs, fresh / whole, 0.0)
    fresh = jnp.broadcast_to(fresh, (group, head)).T
    total = jnp.concatenate([fresh[b * group:(b + 1) * group, 0:1] * new_in[b:b + 1] for b in range(batch)], 0)
    for side, start in enumerate((near, far)):
        arrived(acc_in.at[pl.ds(start, n // 2)], g_recv.at[up if side == 0 else 1 - up])
        for k in range(n // 2):
            j = side * (n // 2) + k
            total = total + weight[:pairs, j:j + 1] * acc_in[start + k].astype(F32)
    for b in range(batch):
        att_rows[b] = total[b * group:(b + 1) * group]
    attended = jnp.concatenate([att_rows[:, h, :].astype(BF16) for h in range(group)], -1)

    arrived(wo, pair_recv.at[0])
    kv_buf[other] = jnp.dot(attended, wo[...], preferred_element_type=F32)
    push(kv_buf.at[other], kv_buf.at[other], send_sem.at[0], pair_recv.at[2], partner)
    arrived(kv_buf.at[kv], pair_recv.at[2])
    out[...] = kv_buf[0] + kv_buf[1]
    sent(a_in, send_sem.at[0])
    sent(b_in, send_sem.at[0])
    sent(a_new, send_sem.at[0])
    sent(b_new, send_sem.at[0])
    sent(wo, send_sem.at[0])
    sent(acc_in, send_sem.at[0])
    sent(stat_in, send_sem.at[0])
    sent(new_in, send_sem.at[0])
    sent(kv_buf.at[0], send_sem.at[0])


def local(n, x, wq, wkv, wo, keys, vals, live, owner):
    batch = x.shape[0]
    head = keys.shape[3]
    slots = keys.shape[2]
    rows, qw = wq.shape
    group = qw // head
    cols = wo.shape[1]
    inner = 1
    while inner * inner < n and n % (inner * 2) == 0:
        inner *= 2
    outer = n // inner
    per = batch // CHUNKS
    half = np.float64(ROPE_THETA) ** (-np.arange(0, head, 2, dtype=np.float64) / head)
    freq = jnp.asarray(np.concatenate([half, half]).astype(np.float32)[None, :])
    dma = pltpu.SemaphoreType.DMA
    vmem = pl.BlockSpec(memory_space=pltpu.VMEM)
    hbm = pl.BlockSpec(memory_space=pl.ANY)
    rounds = max(outer.bit_length() - 2, 1)
    return pl.pallas_call(
        functools.partial(kernel, n, inner, outer, group, head),
        out_shape=pltpu.VMEM((batch, cols), F32),
        in_specs=[hbm] * 9,
        out_specs=vmem,
        scratch_shapes=[
            pltpu.SMEM(live.shape, jnp.int32),
            pltpu.SMEM(owner.shape, jnp.int32),
            pltpu.VMEM((1, head), F32),
            pltpu.VMEM((batch, rows), BF16),
            pltpu.VMEM(wq.shape, BF16),
            pltpu.VMEM(wkv.shape, BF16),
            pltpu.VMEM(wo.shape, BF16),
            pltpu.VMEM(keys.shape, BF16),
            pltpu.VMEM((batch, head, slots), BF16),
            pltpu.VMEM(vals.shape, BF16),
            pltpu.VMEM((batch, group, head), F32),
            pltpu.VMEM((2, batch, head), F32),
            pltpu.VMEM((CHUNKS, inner, per, group, head), F32),
            pltpu.VMEM((inner, 2, batch, head), F32),
            pltpu.VMEM((batch, group, head), F32),
            pltpu.VMEM((2, batch, head), F32),
            pltpu.VMEM((CHUNKS, outer, per, group, head), F32),
            pltpu.VMEM((outer, 2, batch, head), F32),
            pltpu.VMEM((batch * group, head), BF16),
            pltpu.VMEM((n, batch * group, head), BF16),
            pltpu.VMEM((1, head), F32),
            pltpu.VMEM((n, 1, head), F32),
            pltpu.VMEM((batch + 1, head), F32),
            pltpu.VMEM((batch + 1, head), F32),
            pltpu.VMEM((2, batch, cols), F32),
            pltpu.VMEM((batch, group, head), F32),
            dma((2 + PIECES,)),
            dma((CHUNKS + 1,)), dma((CHUNKS + 1,)), dma((2,)),
            dma((1,)),
            dma((4,)),
            pltpu.SemaphoreType.REGULAR((2 + rounds,)),
        ],
        compiler_params=pltpu.CompilerParams(collective_id=0, has_side_effects=True),
    )(live, owner, freq, x, wq, wkv, wo, keys, vals).astype(BF16)


def solution(mesh):
    return jax.shard_map(
        functools.partial(local, mesh.shape["seq"]),
        mesh=mesh,
        in_specs=(
            P("dp", None),
            P("seq", "kv"),
            P("seq", "kv"),
            P("kv", "seq"),
            P("dp", "kv", "seq", None),
            P("dp", "kv", "seq", None),
            P("dp", None),
            P("dp"),
        ),
        out_specs=P("dp", "seq"),
        check_vma=False,
    )
```

```python
import functools
import math

import jax
import jax.numpy as jnp
import numpy as np
from jax import lax
from jax.experimental import pallas as pl
from jax.experimental.pallas import tpu as pltpu
from jax.sharding import PartitionSpec as P

ROPE_THETA = 500000.0
F32 = jnp.float32
BF16 = jnp.bfloat16
MESH = pl.DeviceIdType.MESH
CHUNKS = 2
PIECES = 4


def kernel(
    n, inner, outer, group, head,
    live_hbm, owner_hbm, freq_hbm, x_hbm, wq_hbm, wkv_hbm, wo_hbm, k_hbm, v_hbm,
    out,
    live, owner, freq, x, wq, wkv, wo, keys, keys_t, vals,
    part, part_new, a_in, a_new, a_sum, sum_new, b_in, b_new,
    acc_out, acc_in, stat_out, stat_in, new_out, new_in, kv_buf, att_rows,
    load_sem, a_recv, b_recv, g_recv, send_sem, pair_recv, ready,
):
    me = lax.axis_index("seq")
    kv = lax.axis_index("kv")
    other = 1 - kv
    batch = x.shape[0]
    rows = wq.shape[0]
    qw = wq.shape[1]
    slots = keys.shape[2]
    per = batch // CHUNKS
    pairs = batch * group
    plane = me // inner
    spot = lax.rem(me, inner)
    partner = {"kv": other}
    steps = [1 << i for i in range(outer.bit_length() - 1)]

    def flipped(j):
        return {"seq": j, "kv": other}

    def across(step):
        return {"seq": (plane + step - 2 * step * lax.rem(plane // step, 2)) * inner + spot}

    def signal(sem, device):
        pl.semaphore_signal(sem, inc=1, device_id=device, device_id_type=MESH)

    def push(src, dst, send, recv, device):
        pltpu.make_async_remote_copy(
            src_ref=src, dst_ref=dst, send_sem=send, recv_sem=recv,
            device_id=device, device_id_type=MESH,
        ).start()

    def arrived(buf, recv):
        pltpu.make_async_remote_copy(
            src_ref=buf, dst_ref=buf, send_sem=send_sem.at[0], recv_sem=recv,
            device_id=partner, device_id_type=MESH,
        ).wait_recv()

    def sent(buf, send):
        pltpu.make_async_remote_copy(
            src_ref=buf, dst_ref=buf, send_sem=send, recv_sem=a_recv.at[0],
            device_id=partner, device_id_type=MESH,
        ).wait_send()

    def in_plane(src, dst, send, recv):
        for d in range(inner - 1, -1, -1):
            push(src, dst, send, recv, flipped(plane * inner + lax.bitwise_xor(spot, d)))

    def over_planes(src, dst, send, recv):
        for rank in ranks:
            push(src, dst, send, recv, flipped(rank * inner + spot))

    up = plane // (outer // 2)
    ranks = [up * k + (1 - up) * (outer - 1 - k) for k in range(outer)]
    order = [rank * inner + lax.bitwise_xor(spot, ds) for rank in ranks for ds in range(inner - 1, -1, -1)]
    first = pl.multiple_of(me * rows, rows)
    piece = rows // PIECES
    x_load = pltpu.make_async_copy(x_hbm.at[:, pl.ds(first, rows)], x, load_sem.at[0])
    q_loads = [
        pltpu.make_async_copy(wq_hbm.at[pl.ds(i * piece, piece)], wq.at[pl.ds(i * piece, piece)], load_sem.at[1 + i])
        for i in range(PIECES)
    ]
    kv_load = pltpu.make_async_copy(wkv_hbm, wkv, load_sem.at[1 + PIECES])
    later = [(live_hbm, live), (owner_hbm, owner), (freq_hbm, freq), (k_hbm, keys), (v_hbm, vals)]
    live_load, owner_load, freq_load, k_load, v_load = [
        pltpu.make_async_copy(src, dst, load_sem.at[i]) for i, (src, dst) in enumerate(later)
    ]
    x_load.start()
    for cp in q_loads:
        cp.start()
    kv_load.start()

    barrier = pltpu.get_barrier_semaphore()
    signal(barrier, partner)
    for d in range(1, inner):
        signal(barrier, flipped(plane * inner + lax.rem(spot + d, inner)))
    for step in steps:
        signal(barrier, across(step))

    x_load.wait()
    live_load.start()
    projected = None
    for i, cp in enumerate(q_loads):
        cp.wait()
        if i == 0:
            owner_load.start()
        if i == 1:
            freq_load.start()
        if i == PIECES - 1:
            k_load.start()
            v_load.start()
        term = jnp.dot(x[:, i * piece:(i + 1) * piece], wq[i * piece:(i + 1) * piece, :], preferred_element_type=F32)
        projected = term if projected is None else projected + term
    for h in range(group):
        part[:, h, :] = projected[:, h * head:(h + 1) * head]
    pl.semaphore_wait(barrier, inner + len(steps))
    for step in steps:
        signal(ready.at[2], across(step))

    for c in range(CHUNKS):
        in_plane(part.at[pl.ds(c * per, per)], a_in.at[c, spot], send_sem.at[0], a_recv.at[c])

    kv_load.wait()
    both = jnp.dot(x[...], wkv[...], preferred_element_type=F32)
    part_new[0] = both[:, :head]
    part_new[1] = both[:, head:]
    in_plane(part_new, a_new.at[spot], send_sem.at[0], a_recv.at[CHUNKS])

    push(wo_hbm, wo, send_sem.at[0], pair_recv.at[0], partner)
    live_load.wait()
    owner_load.wait()
    freq_load.wait()
    row_id = lax.broadcasted_iota(jnp.int32, (batch, head), 0)
    lane_id = lax.broadcasted_iota(jnp.int32, (batch, head), 1)
    position = jnp.zeros((batch, head), jnp.int32)
    for b in range(batch):
        own = owner[b]
        position = jnp.where(row_id == b, own * slots + live[b, own], position)
    angle = position.astype(F32) * freq[...]
    cosine = jnp.cos(angle)
    sine = jnp.sin(angle)
    sine = jnp.where(lane_id < head // 2, -sine, sine)

    k_load.wait()
    for b in range(batch):
        keys_t[b] = keys[b, 0].T
    pl.semaphore_wait(ready.at[2], len(steps))
    for i in range(1, len(steps) - 1):
        for step in steps:
            signal(ready.at[2 + i], across(step))
        pl.semaphore_wait(ready.at[2 + i], len(steps))
    signal(ready.at[0], partner)
    pl.semaphore_wait(ready.at[0], 1)

    for c in range(CHUNKS):
        arrived(a_in.at[c], a_recv.at[c])
        total = a_in[c, 0]
        for j in range(1, inner):
            total = total + a_in[c, j]
        a_sum[c * per:(c + 1) * per] = total
        over_planes(a_sum.at[pl.ds(c * per, per)], b_in.at[c, plane], send_sem.at[0], b_recv.at[c])
    arrived(a_new, a_recv.at[CHUNKS])
    total = a_new[0]
    for j in range(1, inner):
        total = total + a_new[j]
    sum_new[...] = total
    v_load.wait()

    scaling = 1.0 / math.sqrt(head)
    slot_id = lax.broadcasted_iota(jnp.int32, (group, slots), 1)
    stat_lane = lax.broadcasted_iota(jnp.int32, (group, head), 1)
    stat_row = lax.broadcasted_iota(jnp.int32, (group, head), 0)
    stat = jnp.zeros((group, head), F32)
    queries = []
    scores = []
    for c in range(CHUNKS):
        arrived(b_in.at[c], b_recv.at[c])
        if c == 0:
            signal(ready.at[1], partner)
            over_planes(sum_new, b_new.at[plane], send_sem.at[0], b_recv.at[CHUNKS])
        total = b_in[c, 0]
        for j in range(1, outer):
            total = total + b_in[c, j]
        for i in range(per):
            b = c * per + i
            q = total[i] * cosine[b:b + 1] + pltpu.roll(total[i], head // 2, 1) * sine[b:b + 1]
            q = q.astype(BF16)
            queries.append(q)
            scores.append(jnp.dot(q, keys_t[b], preferred_element_type=F32))
    accs = []
    for b in range(batch):
        s = jnp.where(slot_id < live[b, me], scores[b] * scaling, -jnp.inf)
        top = jnp.max(s, -1, keepdims=True)
        prob = jnp.exp(s - top).astype(BF16)
        count = jnp.sum(prob.astype(F32), -1, keepdims=True)
        accs.append(jnp.dot(prob, vals[b, 0], preferred_element_type=F32))
        stat = jnp.where(stat_lane == b * group + stat_row, top, stat)
        stat = jnp.where(stat_lane == pairs + b * group + stat_row, count, stat)
    acc_out[...] = jnp.concatenate(accs, 0).astype(BF16)
    stat_out[...] = jnp.sum(stat, 0, keepdims=True)
    pl.semaphore_wait(ready.at[1], 1)
    for side in range(2):
        peers = order[side * n // 2:(side + 1) * n // 2]
        for j in peers:
            push(stat_out, stat_in.at[me], send_sem.at[0], pair_recv.at[3], flipped(j))
        for j in peers:
            push(acc_out, acc_in.at[me], send_sem.at[0], g_recv.at[up], flipped(j))

    arrived(b_new, b_recv.at[CHUNKS])
    total = b_new[0]
    for j in range(1, outer):
        total = total + b_new[j]
    key_new = total[0] * cosine + pltpu.roll(total[0], head // 2, 1) * sine
    key_new = key_new.astype(BF16).astype(F32)
    fresh = jnp.where(stat_lane >= pairs, 1.0 / group, 0.0)
    for b in range(batch):
        score = jnp.sum(queries[b].astype(F32) * key_new[b:b + 1], -1, keepdims=True) * scaling
        fresh = jnp.where(stat_lane == b * group + stat_row, score, fresh)
    new_out[:batch] = total[1].astype(BF16).astype(F32)
    new_out[batch:batch + 1] = jnp.sum(fresh, 0, keepdims=True)
    push(new_out, new_in, send_sem.at[0], pair_recv.at[1], partner)

    arrived(stat_in, pair_recv.at[3])
    arrived(new_in, pair_recv.at[1])
    near = pl.multiple_of(up * (n // 2), n // 2)
    far = pl.multiple_of((1 - up) * (n // 2), n // 2)
    stats = jnp.concatenate([stat_in[pl.ds(near, n // 2), 0, :], stat_in[pl.ds(far, n // 2), 0, :]], 0)
    newest = new_in[batch:batch + 1]
    top = jnp.maximum(jnp.max(stats, 0, keepdims=True), newest)
    factor = jnp.exp(stats - top)
    fresh = jnp.exp(newest - top)
    whole = jnp.sum(factor * pltpu.roll(stats, head - pairs, 1), 0, keepdims=True) + fresh
    lane = lax.broadcasted_iota(jnp.int32, stats.shape, 1)
    weight = jnp.where(lane < pairs, factor / whole, 0.0).T
    fresh = jnp.where(lane[:1] < pairs, fresh / whole, 0.0)
    fresh = jnp.broadcast_to(fresh, (group, head)).T
    total = jnp.concatenate([fresh[b * group:(b + 1) * group, 0:1] * new_in[b:b + 1] for b in range(batch)], 0)
    for side, start in enumerate((near, far)):
        arrived(acc_in.at[pl.ds(start, n // 2)], g_recv.at[up if side == 0 else 1 - up])
        for k in range(n // 2):
            j = side * (n // 2) + k
            total = total + weight[:pairs, j:j + 1] * acc_in[start + k].astype(F32)
    for b in range(batch):
        att_rows[b] = total[b * group:(b + 1) * group]
    attended = jnp.concatenate([att_rows[:, h, :].astype(BF16) for h in range(group)], -1)

    arrived(wo, pair_recv.at[0])
    kv_buf[other] = jnp.dot(attended, wo[...], preferred_element_type=F32)
    push(kv_buf.at[other], kv_buf.at[other], send_sem.at[0], pair_recv.at[2], partner)
    arrived(kv_buf.at[kv], pair_recv.at[2])
    out[...] = kv_buf[0] + kv_buf[1]
    sent(a_in, send_sem.at[0])
    sent(b_in, send_sem.at[0])
    sent(a_new, send_sem.at[0])
    sent(b_new, send_sem.at[0])
    sent(wo, send_sem.at[0])
    sent(acc_in, send_sem.at[0])
    sent(stat_in, send_sem.at[0])
    sent(new_in, send_sem.at[0])
    sent(kv_buf.at[0], send_sem.at[0])


def local(n, x, wq, wkv, wo, keys, vals, live, owner):
    batch = x.shape[0]
    head = keys.shape[3]
    slots = keys.shape[2]
    rows, qw = wq.shape
    group = qw // head
    cols = wo.shape[1]
    inner = 1
    while inner * inner < n and n % (inner * 2) == 0:
        inner *= 2
    outer = n // inner
    per = batch // CHUNKS
    half = np.float64(ROPE_THETA) ** (-np.arange(0, head, 2, dtype=np.float64) / head)
    freq = jnp.asarray(np.concatenate([half, half]).astype(np.float32)[None, :])
    dma = pltpu.SemaphoreType.DMA
    vmem = pl.BlockSpec(memory_space=pltpu.VMEM)
    hbm = pl.BlockSpec(memory_space=pl.ANY)
    rounds = max(outer.bit_length() - 2, 1)
    return pl.pallas_call(
        functools.partial(kernel, n, inner, outer, group, head),
        out_shape=pltpu.VMEM((batch, cols), F32),
        in_specs=[hbm] * 9,
        out_specs=vmem,
        scratch_shapes=[
            pltpu.SMEM(live.shape, jnp.int32),
            pltpu.SMEM(owner.shape, jnp.int32),
            pltpu.VMEM((1, head), F32),
            pltpu.VMEM((batch, rows), BF16),
            pltpu.VMEM(wq.shape, BF16),
            pltpu.VMEM(wkv.shape, BF16),
            pltpu.VMEM(wo.shape, BF16),
            pltpu.VMEM(keys.shape, BF16),
            pltpu.VMEM((batch, head, slots), BF16),
            pltpu.VMEM(vals.shape, BF16),
            pltpu.VMEM((batch, group, head), F32),
            pltpu.VMEM((2, batch, head), F32),
            pltpu.VMEM((CHUNKS, inner, per, group, head), F32),
            pltpu.VMEM((inner, 2, batch, head), F32),
            pltpu.VMEM((batch, group, head), F32),
            pltpu.VMEM((2, batch, head), F32),
            pltpu.VMEM((CHUNKS, outer, per, group, head), F32),
            pltpu.VMEM((outer, 2, batch, head), F32),
            pltpu.VMEM((batch * group, head), BF16),
            pltpu.VMEM((n, batch * group, head), BF16),
            pltpu.VMEM((1, head), F32),
            pltpu.VMEM((n, 1, head), F32),
            pltpu.VMEM((batch + 1, head), F32),
            pltpu.VMEM((batch + 1, head), F32),
            pltpu.VMEM((2, batch, cols), F32),
            pltpu.VMEM((batch, group, head), F32),
            dma((2 + PIECES,)),
            dma((CHUNKS + 1,)), dma((CHUNKS + 1,)), dma((2,)),
            dma((1,)),
            dma((4,)),
            pltpu.SemaphoreType.REGULAR((2 + rounds,)),
        ],
        compiler_params=pltpu.CompilerParams(collective_id=0, has_side_effects=True),
    )(live, owner, freq, x, wq, wkv, wo, keys, vals).astype(BF16)


def solution(mesh):
    return jax.shard_map(
        functools.partial(local, mesh.shape["seq"]),
        mesh=mesh,
        in_specs=(
            P("dp", None),
            P("seq", "kv"),
            P("seq", "kv"),
            P("kv", "seq"),
            P("dp", "kv", "seq", None),
            P("dp", "kv", "seq", None),
            P("dp", None),
            P("dp"),
        ),
        out_specs=P("dp", "seq"),
        check_vma=False,
    )
```

```python
import functools
import math

import jax
import jax.numpy as jnp
import numpy as np
from jax import lax
from jax.experimental import pallas as pl
from jax.experimental.pallas import tpu as pltpu
from jax.sharding import PartitionSpec as P

ROPE_THETA = 500000.0
F32 = jnp.float32
BF16 = jnp.bfloat16
MESH = pl.DeviceIdType.MESH
CHUNKS = 2
PIECES = 4


def kernel(
    n, inner, outer, group, head,
    live_hbm, owner_hbm, freq_hbm, x_hbm, wq_hbm, wkv_hbm, wo_hbm, k_hbm, v_hbm,
    out,
    live, owner, freq, x, wq, wkv, wo, keys, keys_t, vals,
    part, part_new, a_in, a_new, a_sum, sum_new, b_in, b_new,
    acc_out, acc_in, stat_out, stat_in, new_out, new_in, kv_buf, att_rows,
    load_sem, a_recv, b_recv, g_recv, send_sem, pair_recv, ready,
):
    me = lax.axis_index("seq")
    kv = lax.axis_index("kv")
    other = 1 - kv
    batch = x.shape[0]
    rows = wq.shape[0]
    qw = wq.shape[1]
    slots = keys.shape[2]
    per = batch // CHUNKS
    pairs = batch * group
    plane = me // inner
    spot = lax.rem(me, inner)
    partner = {"kv": other}
    steps = [1 << i for i in range(outer.bit_length() - 1)]

    def flipped(j):
        return {"seq": j, "kv": other}

    def across(step):
        return {"seq": (plane + step - 2 * step * lax.rem(plane // step, 2)) * inner + spot}

    def signal(sem, device):
        pl.semaphore_signal(sem, inc=1, device_id=device, device_id_type=MESH)

    def push(src, dst, send, recv, device):
        pltpu.make_async_remote_copy(
            src_ref=src, dst_ref=dst, send_sem=send, recv_sem=recv,
            device_id=device, device_id_type=MESH,
        ).start()

    def arrived(buf, recv):
        pltpu.make_async_remote_copy(
            src_ref=buf, dst_ref=buf, send_sem=send_sem.at[0], recv_sem=recv,
            device_id=partner, device_id_type=MESH,
        ).wait_recv()

    def sent(buf, send):
        pltpu.make_async_remote_copy(
            src_ref=buf, dst_ref=buf, send_sem=send, recv_sem=a_recv.at[0],
            device_id=partner, device_id_type=MESH,
        ).wait_send()

    def in_plane(src, dst, send, recv):
        for d in range(inner - 1, -1, -1):
            push(src, dst, send, recv, flipped(plane * inner + lax.bitwise_xor(spot, d)))

    def over_planes(src, dst, send, recv):
        for rank in ranks:
            push(src, dst, send, recv, flipped(rank * inner + spot))

    up = plane // (outer // 2)
    ranks = [up * k + (1 - up) * (outer - 1 - k) for k in range(outer)]
    order = [rank * inner + lax.bitwise_xor(spot, ds) for rank in ranks for ds in range(inner - 1, -1, -1)]
    first = pl.multiple_of(me * rows, rows)
    piece = rows // PIECES
    x_load = pltpu.make_async_copy(x_hbm.at[:, pl.ds(first, rows)], x, load_sem.at[0])
    q_loads = [
        pltpu.make_async_copy(wq_hbm.at[pl.ds(i * piece, piece)], wq.at[pl.ds(i * piece, piece)], load_sem.at[1 + i])
        for i in range(PIECES)
    ]
    kv_load = pltpu.make_async_copy(wkv_hbm, wkv, load_sem.at[1 + PIECES])
    later = [(live_hbm, live), (owner_hbm, owner), (freq_hbm, freq), (k_hbm, keys), (v_hbm, vals)]
    live_load, owner_load, freq_load, k_load, v_load = [
        pltpu.make_async_copy(src, dst, load_sem.at[i]) for i, (src, dst) in enumerate(later)
    ]
    x_load.start()
    for cp in q_loads:
        cp.start()
    kv_load.start()

    barrier = pltpu.get_barrier_semaphore()
    signal(barrier, partner)
    for d in range(1, inner):
        signal(barrier, flipped(plane * inner + lax.rem(spot + d, inner)))
    for step in steps:
        signal(barrier, across(step))

    x_load.wait()
    live_load.start()
    projected = None
    for i, cp in enumerate(q_loads):
        cp.wait()
        if i == 0:
            owner_load.start()
        if i == 1:
            freq_load.start()
        if i == PIECES - 1:
            k_load.start()
            v_load.start()
        term = jnp.dot(x[:, i * piece:(i + 1) * piece], wq[i * piece:(i + 1) * piece, :], preferred_element_type=F32)
        projected = term if projected is None else projected + term
    for h in range(group):
        part[:, h, :] = projected[:, h * head:(h + 1) * head]
    pl.semaphore_wait(barrier, inner + len(steps))
    for step in steps:
        signal(ready.at[2], across(step))

    for c in range(CHUNKS):
        in_plane(part.at[pl.ds(c * per, per)], a_in.at[c, spot], send_sem.at[0], a_recv.at[c])

    kv_load.wait()
    both = jnp.dot(x[...], wkv[...], preferred_element_type=F32)
    part_new[0] = both[:, :head]
    part_new[1] = both[:, head:]
    in_plane(part_new, a_new.at[spot], send_sem.at[0], a_recv.at[CHUNKS])

    push(wo_hbm, wo, send_sem.at[0], pair_recv.at[0], partner)
    live_load.wait()
    owner_load.wait()
    freq_load.wait()
    row_id = lax.broadcasted_iota(jnp.int32, (batch, head), 0)
    lane_id = lax.broadcasted_iota(jnp.int32, (batch, head), 1)
    position = jnp.zeros((batch, head), jnp.int32)
    for b in range(batch):
        own = owner[b]
        position = jnp.where(row_id == b, own * slots + live[b, own], position)
    angle = position.astype(F32) * freq[...]
    cosine = jnp.cos(angle)
    sine = jnp.sin(angle)
    sine = jnp.where(lane_id < head // 2, -sine, sine)

    k_load.wait()
    for b in range(batch):
        keys_t[b] = keys[b, 0].T
    pl.semaphore_wait(ready.at[2], len(steps))
    for i in range(1, len(steps) - 1):
        for step in steps:
            signal(ready.at[2 + i], across(step))
        pl.semaphore_wait(ready.at[2 + i], len(steps))
    signal(ready.at[0], partner)
    pl.semaphore_wait(ready.at[0], 1)

    for c in range(CHUNKS):
        arrived(a_in.at[c], a_recv.at[c])
        total = a_in[c, 0]
        for j in range(1, inner):
            total = total + a_in[c, j]
        a_sum[c * per:(c + 1) * per] = total
        over_planes(a_sum.at[pl.ds(c * per, per)], b_in.at[c, plane], send_sem.at[0], b_recv.at[c])
    arrived(a_new, a_recv.at[CHUNKS])
    total = a_new[0]
    for j in range(1, inner):
        total = total + a_new[j]
    sum_new[...] = total
    v_load.wait()

    scaling = 1.0 / math.sqrt(head)
    slot_id = lax.broadcasted_iota(jnp.int32, (group, slots), 1)
    stat_lane = lax.broadcasted_iota(jnp.int32, (group, head), 1)
    stat_row = lax.broadcasted_iota(jnp.int32, (group, head), 0)
    stat = jnp.zeros((group, head), F32)
    queries = []
    scores = []
    for c in range(CHUNKS):
        arrived(b_in.at[c], b_recv.at[c])
        if c == 0:
            signal(ready.at[1], partner)
            over_planes(sum_new, b_new.at[plane], send_sem.at[0], b_recv.at[CHUNKS])
        total = b_in[c, 0]
        for j in range(1, outer):
            total = total + b_in[c, j]
        for i in range(per):
            b = c * per + i
            q = total[i] * cosine[b:b + 1] + pltpu.roll(total[i], head // 2, 1) * sine[b:b + 1]
            q = q.astype(BF16)
            queries.append(q)
            scores.append(jnp.dot(q, keys_t[b], preferred_element_type=F32))
    accs = []
    for b in range(batch):
        s = jnp.where(slot_id < live[b, me], scores[b] * scaling, -jnp.inf)
        top = jnp.max(s, -1, keepdims=True)
        prob = jnp.exp(s - top).astype(BF16)
        count = jnp.sum(prob.astype(F32), -1, keepdims=True)
        accs.append(jnp.dot(prob, vals[b, 0], preferred_element_type=F32))
        stat = jnp.where(stat_lane == b * group + stat_row, top, stat)
        stat = jnp.where(stat_lane == pairs + b * group + stat_row, count, stat)
    acc_out[...] = jnp.concatenate(accs, 0).astype(BF16)
    stat_out[...] = jnp.sum(stat, 0, keepdims=True)
    pl.semaphore_wait(ready.at[1], 1)
    for side in range(2):
        peers = order[side * n // 2:(side + 1) * n // 2]
        for j in peers[len(peers) // 2:] + peers[:len(peers) // 2]:
            push(stat_out, stat_in.at[me], send_sem.at[0], pair_recv.at[3], flipped(j))
        for j in peers:
            push(acc_out, acc_in.at[me], send_sem.at[0], g_recv.at[up], flipped(j))

    arrived(b_new, b_recv.at[CHUNKS])
    total = b_new[0]
    for j in range(1, outer):
        total = total + b_new[j]
    key_new = total[0] * cosine + pltpu.roll(total[0], head // 2, 1) * sine
    key_new = key_new.astype(BF16).astype(F32)
    fresh = jnp.where(stat_lane >= pairs, 1.0 / group, 0.0)
    for b in range(batch):
        score = jnp.sum(queries[b].astype(F32) * key_new[b:b + 1], -1, keepdims=True) * scaling
        fresh = jnp.where(stat_lane == b * group + stat_row, score, fresh)
    new_out[:batch] = total[1].astype(BF16).astype(F32)
    new_out[batch:batch + 1] = jnp.sum(fresh, 0, keepdims=True)
    push(new_out, new_in, send_sem.at[0], pair_recv.at[1], partner)

    arrived(stat_in, pair_recv.at[3])
    arrived(new_in, pair_recv.at[1])
    near = pl.multiple_of(up * (n // 2), n // 2)
    far = pl.multiple_of((1 - up) * (n // 2), n // 2)
    stats = jnp.concatenate([stat_in[pl.ds(near, n // 2), 0, :], stat_in[pl.ds(far, n // 2), 0, :]], 0)
    newest = new_in[batch:batch + 1]
    top = jnp.maximum(jnp.max(stats, 0, keepdims=True), newest)
    factor = jnp.exp(stats - top)
    fresh = jnp.exp(newest - top)
    whole = jnp.sum(factor * pltpu.roll(stats, head - pairs, 1), 0, keepdims=True) + fresh
    lane = lax.broadcasted_iota(jnp.int32, stats.shape, 1)
    weight = jnp.where(lane < pairs, factor / whole, 0.0).T
    fresh = jnp.where(lane[:1] < pairs, fresh / whole, 0.0)
    fresh = jnp.broadcast_to(fresh, (group, head)).T
    total = jnp.concatenate([fresh[b * group:(b + 1) * group, 0:1] * new_in[b:b + 1] for b in range(batch)], 0)
    for side, start in enumerate((near, far)):
        arrived(acc_in.at[pl.ds(start, n // 2)], g_recv.at[up if side == 0 else 1 - up])
        for k in range(n // 2):
            j = side * (n // 2) + k
            total = total + weight[:pairs, j:j + 1] * acc_in[start + k].astype(F32)
    for b in range(batch):
        att_rows[b] = total[b * group:(b + 1) * group]
    attended = jnp.concatenate([att_rows[:, h, :].astype(BF16) for h in range(group)], -1)

    arrived(wo, pair_recv.at[0])
    kv_buf[other] = jnp.dot(attended, wo[...], preferred_element_type=F32)
    push(kv_buf.at[other], kv_buf.at[other], send_sem.at[0], pair_recv.at[2], partner)
    arrived(kv_buf.at[kv], pair_recv.at[2])
    out[...] = kv_buf[0] + kv_buf[1]
    sent(a_in, send_sem.at[0])
    sent(b_in, send_sem.at[0])
    sent(a_new, send_sem.at[0])
    sent(b_new, send_sem.at[0])
    sent(wo, send_sem.at[0])
    sent(acc_in, send_sem.at[0])
    sent(stat_in, send_sem.at[0])
    sent(new_in, send_sem.at[0])
    sent(kv_buf.at[0], send_sem.at[0])


def local(n, x, wq, wkv, wo, keys, vals, live, owner):
    batch = x.shape[0]
    head = keys.shape[3]
    slots = keys.shape[2]
    rows, qw = wq.shape
    group = qw // head
    cols = wo.shape[1]
    inner = 1
    while inner * inner < n and n % (inner * 2) == 0:
        inner *= 2
    outer = n // inner
    per = batch // CHUNKS
    half = np.float64(ROPE_THETA) ** (-np.arange(0, head, 2, dtype=np.float64) / head)
    freq = jnp.asarray(np.concatenate([half, half]).astype(np.float32)[None, :])
    dma = pltpu.SemaphoreType.DMA
    vmem = pl.BlockSpec(memory_space=pltpu.VMEM)
    hbm = pl.BlockSpec(memory_space=pl.ANY)
    rounds = max(outer.bit_length() - 2, 1)
    return pl.pallas_call(
        functools.partial(kernel, n, inner, outer, group, head),
        out_shape=pltpu.VMEM((batch, cols), F32),
        in_specs=[hbm] * 9,
        out_specs=vmem,
        scratch_shapes=[
            pltpu.SMEM(live.shape, jnp.int32),
            pltpu.SMEM(owner.shape, jnp.int32),
            pltpu.VMEM((1, head), F32),
            pltpu.VMEM((batch, rows), BF16),
            pltpu.VMEM(wq.shape, BF16),
            pltpu.VMEM(wkv.shape, BF16),
            pltpu.VMEM(wo.shape, BF16),
            pltpu.VMEM(keys.shape, BF16),
            pltpu.VMEM((batch, head, slots), BF16),
            pltpu.VMEM(vals.shape, BF16),
            pltpu.VMEM((batch, group, head), F32),
            pltpu.VMEM((2, batch, head), F32),
            pltpu.VMEM((CHUNKS, inner, per, group, head), F32),
            pltpu.VMEM((inner, 2, batch, head), F32),
            pltpu.VMEM((batch, group, head), F32),
            pltpu.VMEM((2, batch, head), F32),
            pltpu.VMEM((CHUNKS, outer, per, group, head), F32),
            pltpu.VMEM((outer, 2, batch, head), F32),
            pltpu.VMEM((batch * group, head), BF16),
            pltpu.VMEM((n, batch * group, head), BF16),
            pltpu.VMEM((1, head), F32),
            pltpu.VMEM((n, 1, head), F32),
            pltpu.VMEM((batch + 1, head), F32),
            pltpu.VMEM((batch + 1, head), F32),
            pltpu.VMEM((2, batch, cols), F32),
            pltpu.VMEM((batch, group, head), F32),
            dma((2 + PIECES,)),
            dma((CHUNKS + 1,)), dma((CHUNKS + 1,)), dma((2,)),
            dma((1,)),
            dma((4,)),
            pltpu.SemaphoreType.REGULAR((2 + rounds,)),
        ],
        compiler_params=pltpu.CompilerParams(collective_id=0, has_side_effects=True),
    )(live, owner, freq, x, wq, wkv, wo, keys, vals).astype(BF16)


def solution(mesh):
    return jax.shard_map(
        functools.partial(local, mesh.shape["seq"]),
        mesh=mesh,
        in_specs=(
            P("dp", None),
            P("seq", "kv"),
            P("seq", "kv"),
            P("kv", "seq"),
            P("dp", "kv", "seq", None),
            P("dp", "kv", "seq", None),
            P("dp", None),
            P("dp"),
        ),
        out_specs=P("dp", "seq"),
        check_vma=False,
    )
```
